128 devices in a mesh: hst: 8 (over y, core), dev: 16 (over z, x).
Axes of the slice: x: 4, y: 4, z: 4, core: 2. Of those that a mesh axis runs over, the one named last changes fastest.
Arguments:
- hot_rows: bfloat16 [4096, 768], replicated, may hold values from -6 to 6
- cold_rows: bfloat16 [131072, 768], P(('hst', 'dev')), may hold values from -6 to 6
- hot_mask: int32 [262144], P(('hst', 'dev')), may hold values from 0 to 1, as said below
- hot_id: int32 [262144], P(('hst', 'dev')), may hold values from 0 to 4095
- cold_owner: int32 [262144], P(('hst', 'dev')), may hold values from 0 to 127, as said below
- cold_pos: int32 [262144], P(('hst', 'dev')), may hold values from 0 to 15, as said below
- cold_send: int32 [128, 2048], P(('hst', 'dev')), may hold values from 0 to 1023
- adjacency_one: int32 [262144, 15], P(('hst', 'dev')), may hold values from 0 to 2047
- adjacency_two: int32 [65536, 15], P(('hst', 'dev')), may hold values from 0 to 2559
- halo_send: int32 [128, 512], P(('hst', 'dev')), may hold values from 0 to 2047
- self_first: bfloat16 [768, 1024], replicated, may hold values from -0.21875 to 0.21875
- neigh_first: bfloat16 [768, 1024], replicated, may hold values from -0.21875 to 0.21875
- bn_gain: float32 [1024], replicated, may hold values from 0.1 to 1.9
- bn_shift: float32 [1024], replicated, may hold values from -3 to 3
- self_second: bfloat16 [1024, 153], replicated, may hold values from -0.1875 to 0.1875
- neigh_second: bfloat16 [1024, 153], replicated, may hold values from -0.1875 to 0.1875
Outputs:
- logits: float32 [65536, 153], P(('hst', 'dev'))
The draws below stay inside these ranges and needn't reach their ends.
Inputs may be any that keep to these rules, and one draw needn't show every extreme that they name: Each device has exactly 1536 nodes with hot_mask 0. `cold_owner`: for each device and owner, at most 16 of the device's nodes with hot_mask 0 name that owner; some owner is named by exactly 16 of them on every device. `cold_pos`: the nodes of one device with hot_mask 0 and the same owner have distinct slots.
All inputs are finite; a program needn't handle non-finite values.
Results may differ from the reference program's by a relative error of at most 0.003.
The reference program's roundings to bfloat16 on the way (of `features`, `first_mean`, `hidden`, `table` and `second_mean`) count: a program that leaves them out, or rounds other values in their place, can miss the bound.
Values may be sent and summed in bfloat16 or wider, within the bound.
No kernel may reach another device: no remote copies, remote signals or barrier semaphores. Data moves between devices by JAX's collectives and lax.ppermute only.
A program may use at most 128 MiB of HBM per device.

```python
import math
import jax
import jax.numpy as jnp
import numpy as np
from jax import lax

F = 768
H = 1024
C = 153
L_DEV = 2048
COLD_DEV = 1024
HCAP = 32
HOT = 4096
K1 = 15
K2 = 15
COLD_NODES = 1536
B_DEV = 512
CAP = 16
NODES = 262144
TARGETS = 65536
COLD_ROWS = 131072
N_HST = 8
N_DEV = 16
DEVICES = 128


def cold_layout(key):
    base = jax.random.fold_in(key, 7)
    key_slots, key_nodes = jax.random.split(base)
    total_slots = DEVICES * CAP
    slot_index = jnp.arange(total_slots, dtype=jnp.int32)
    noise = jax.random.randint(key_slots, (DEVICES, total_slots), 0, 2 ** 19, dtype=jnp.int32)
    scores = noise * total_slots + slot_index[None, :]
    forced = (slot_index // CAP)[None, :] == ((jnp.arange(DEVICES, dtype=jnp.int32) + 1) % DEVICES)[:, None]
    scores = jnp.where(forced, slot_index[None, :] - total_slots, scores)
    chosen = jnp.argsort(scores, axis=1)[:, :COLD_NODES].astype(jnp.int32)
    owners = chosen // CAP
    positions = chosen % CAP
    node_noise = jax.random.randint(key_nodes, (DEVICES, L_DEV), 0, 2 ** 19, dtype=jnp.int32)
    node_scores = node_noise * L_DEV + jnp.arange(L_DEV, dtype=jnp.int32)[None, :]
    order = jnp.argsort(node_scores, axis=1)[:, :COLD_NODES].astype(jnp.int32)
    device_rows = jnp.broadcast_to(jnp.arange(DEVICES, dtype=jnp.int32)[:, None], order.shape)
    owner_full = jnp.zeros((DEVICES, L_DEV), jnp.int32).at[device_rows, order].set(owners)
    pos_full = jnp.zeros((DEVICES, L_DEV), jnp.int32).at[device_rows, order].set(positions)
    cold_flag = jnp.zeros((DEVICES, L_DEV), jnp.int32).at[device_rows, order].set(1)
    return (owner_full.reshape(-1), pos_full.reshape(-1), (1 - cold_flag).reshape(-1))


def draw_hot_mask(key, part):
    return cold_layout(key)[2]


def draw_cold_owner(key, part):
    return cold_layout(key)[0]


def draw_cold_pos(key, part):
    return cold_layout(key)[1]


def with_ends(drawn, rng, low, top_value):
    dims = drawn.shape
    place = [jax.random.randint(jax.random.fold_in(rng, axis), (), 0, dims[axis]) for axis in range(len(dims))]
    drawn = drawn.at[tuple(place)].set(low)
    longest = dims.index(max(dims))
    place[longest] = (place[longest] + 1) % dims[longest]
    return drawn.at[tuple(place)].set(top_value)


def shard_levels(rng, extent, pieces, low, high):
    level, own = 1.0, jax.random.fold_in(rng, 6)
    for dim, parts in pieces:
        draws = jnp.exp(jax.random.uniform(jax.random.fold_in(own, dim), (parts,), jnp.float32, low / len(pieces), high / len(pieces)))
        level = level * jnp.repeat(draws, extent[dim] // parts).reshape([-1 if axis == dim else 1 for axis in range(len(extent))])
    return level


def rank_table(count, slope):
    weights = [(1 << 20) // math.isqrt(standing ** slope) + 1 for standing in range(1, count + 1)]
    width = 1 + sum(weights) // (1 << 30)
    return np.cumsum(np.array([max(1, weight // width) for weight in weights]))


def ranked(own_key, dims, amount, skew):
    listing = rank_table(amount, skew)
    pick = jax.random.randint(jax.random.fold_in(own_key, 1), dims, 0, int(listing[amount - 1]))
    rank = jnp.searchsorted(jnp.asarray(listing, jnp.int32), pick, side="right")
    return jax.random.permutation(jax.random.fold_in(own_key, 2), amount)[rank].astype(jnp.int32)


def gaussian(rng, dims, deviation, bound, shards=(), kind=jnp.bfloat16):
    level = shard_levels(rng, dims, shards, -0.22, 0.18) if shards else 1.0
    values = jax.random.normal(rng, dims, jnp.float32) * deviation * level
    return jnp.minimum(jnp.maximum(values, -bound), bound).astype(kind)


def setup_inputs(seed: int = 0) -> dict:
    arg_keys = jax.random.split(jax.random.key(seed), 17)
    hot_rows = gaussian(arg_keys[0], (HOT, F), 1.0, 6.0)
    cold_rows = gaussian(arg_keys[1], (COLD_ROWS, F), 1.0, 6.0, ((0, 128),))
    hot_mask = draw_hot_mask(jax.random.fold_in(arg_keys[16], 71), 0)
    hot_id = with_ends(ranked(arg_keys[3], (NODES,), HOT, 2), jax.random.fold_in(arg_keys[3], 3), 0, HOT - 1).astype(jnp.int32)
    cold_owner = draw_cold_owner(jax.random.fold_in(arg_keys[16], 71), 0)
    cold_pos = draw_cold_pos(jax.random.fold_in(arg_keys[16], 71), 0)
    cold_send = with_ends(jax.random.randint(arg_keys[6], (DEVICES, DEVICES * CAP), 0, COLD_DEV), jax.random.fold_in(arg_keys[6], 1), 0, COLD_DEV - 1).astype(jnp.int32)
    adjacency_one = with_ends(jax.random.randint(arg_keys[7], (NODES, K1), 0, L_DEV), jax.random.fold_in(arg_keys[7], 1), 0, L_DEV - 1).astype(jnp.int32)
    adjacency_two = with_ends(jax.random.randint(arg_keys[8], (TARGETS, K2), 0, L_DEV + N_DEV * HCAP), jax.random.fold_in(arg_keys[8], 1), 0, (L_DEV + N_DEV * HCAP) - 1).astype(jnp.int32)
    halo_send = with_ends(jax.random.randint(arg_keys[9], (DEVICES, N_DEV * HCAP), 0, L_DEV), jax.random.fold_in(arg_keys[9], 1), 0, L_DEV - 1).astype(jnp.int32)
    self_first = gaussian(arg_keys[10], (F, H), F ** -0.5, 0.21875)
    neigh_first = gaussian(arg_keys[11], (F, H), F ** -0.5, 0.21875)
    bn_gain = jnp.clip(1.0 + 0.18 * jax.random.normal(arg_keys[12], (H,), jnp.float32), 0.1, 1.9)
    bn_shift = gaussian(arg_keys[13], (H,), 0.5, 3.0, (), jnp.float32)
    self_second = gaussian(arg_keys[14], (H, C), H ** -0.5, 0.1875)
    neigh_second = gaussian(arg_keys[15], (H, C), H ** -0.5, 0.1875)
    return {"hot_rows": hot_rows, "cold_rows": cold_rows, "hot_mask": hot_mask, "hot_id": hot_id, "cold_owner": cold_owner, "cold_pos": cold_pos, "cold_send": cold_send, "adjacency_one": adjacency_one, "adjacency_two": adjacency_two, "halo_send": halo_send, "self_first": self_first, "neigh_first": neigh_first, "bn_gain": bn_gain, "bn_shift": bn_shift, "self_second": self_second, "neigh_second": neigh_second}


epsilon = 1e-05

def gather_mean(table, neighbours, fanout):
    total = jnp.zeros((neighbours.shape[0], table.shape[1]), jnp.float32)
    for column in range(fanout):
        total = total + jnp.take(table, neighbours[:, column], axis=0).astype(jnp.float32)
    return (total / fanout).astype(jnp.bfloat16)

def reference(hot_rows, cold_rows, hot_mask, hot_id, cold_owner, cold_pos, cold_send, adjacency_one, adjacency_two, halo_send, self_first, neigh_first, bn_gain, bn_shift, self_second, neigh_second):
    devices = N_HST * N_DEV

    def first_layer(device):
        start = (device * L_DEV).astype(jnp.int32)
        mask_here = lax.dynamic_slice_in_dim(hot_mask, start, L_DEV)
        hot_here = lax.dynamic_slice_in_dim(hot_id, start, L_DEV)
        owner_here = lax.dynamic_slice_in_dim(cold_owner, start, L_DEV)
        pos_here = lax.dynamic_slice_in_dim(cold_pos, start, L_DEV)
        nbrs_here = lax.dynamic_slice_in_dim(adjacency_one, start, L_DEV)
        slot = cold_send[owner_here, (device * CAP + pos_here).astype(jnp.int32)]
        cold_feat = jnp.take(cold_rows, (owner_here * COLD_DEV + slot).astype(jnp.int32), axis=0)
        hot_feat = jnp.take(hot_rows, hot_here, axis=0)
        features = jnp.where(mask_here[:, None] == 1, hot_feat, cold_feat)
        first_mean = gather_mean(features, nbrs_here, K1)
        return jnp.dot(features, self_first, preferred_element_type=jnp.float32) + jnp.dot(first_mean, neigh_first, preferred_element_type=jnp.float32)
    hidden_pre = lax.map(first_layer, jnp.arange(devices, dtype=jnp.int32))
    mean = lax.optimization_barrier(jnp.mean(hidden_pre, axis=(0, 1)))
    variance = lax.optimization_barrier(jnp.mean(jnp.square(hidden_pre - mean), axis=(0, 1)))
    hidden = jax.nn.relu((hidden_pre - mean) * lax.rsqrt(variance + epsilon) * bn_gain + bn_shift).astype(jnp.bfloat16)
    sends = halo_send.reshape(devices, N_DEV, HCAP)

    def second_layer(device):
        group = device // N_DEV
        lane = device % N_DEV
        peers = (group * N_DEV + jnp.arange(N_DEV, dtype=jnp.int32)).astype(jnp.int32)
        picks = sends[peers, lane]
        boundary = hidden[peers[:, None], picks].reshape(N_DEV * HCAP, H)
        own = lax.dynamic_index_in_dim(hidden, device, 0, keepdims=False)
        table = jnp.concatenate([own, boundary], axis=0)
        nbrs_here = lax.dynamic_slice_in_dim(adjacency_two, (device * B_DEV).astype(jnp.int32), B_DEV)
        second_mean = gather_mean(table, nbrs_here, K2)
        return jnp.dot(own[:B_DEV], self_second, preferred_element_type=jnp.float32) + jnp.dot(second_mean, neigh_second, preferred_element_type=jnp.float32)
    logits = lax.map(second_layer, jnp.arange(devices, dtype=jnp.int32))
    return logits.reshape(devices * B_DEV, C)
```

```python
import functools

import jax
import jax.numpy as jnp
from jax import lax
from jax.experimental import pallas as pl
from jax.experimental.pallas import tpu as pltpu
from jax.sharding import Mesh
from jax.sharding import PartitionSpec as P

HST = ("hst_0", "hst_1")
DEV = ("dev_0", "dev_1")
HST_DEV = ("hst_0", "hst_1", "dev_0", "dev_1")

LANES = 128
BLOCK = 512
epsilon = 1e-05

f32 = jnp.float32
bf16 = jnp.bfloat16


def row_to_lanes(row):
    return jnp.transpose(jnp.broadcast_to(row, (LANES, row.shape[1])))


def one_hot(row, width):
    spread = row_to_lanes(row).astype(jnp.int16)
    lane = lax.broadcasted_iota(jnp.int32, spread.shape, 1).astype(jnp.int16)
    one, zero = jnp.array(1, bf16), jnp.array(0, bf16)
    tiles = [
        jnp.where(spread == lane + jnp.int16(LANES * j), one, zero) for j in range(width // LANES)
    ]
    return jnp.concatenate(tiles, axis=1)


def params(**kw):
    return pltpu.CompilerParams(dimension_semantics=("arbitrary",), vmem_limit_bytes=60 * 2**20, **kw)


def whole(shape):
    return pl.BlockSpec(shape, lambda i: (0,) * len(shape))


def select_rows_kernel(idx_ref, table_ref, out_ref):
    hot = one_hot(idx_ref[...], table_ref.shape[0])
    out_ref[...] = jnp.dot(hot, table_ref[...], preferred_element_type=f32).astype(bf16)


def select_rows(idx, table):
    rows, width = idx.shape[1], table.shape[1]
    return pl.pallas_call(
        select_rows_kernel,
        grid=(rows // BLOCK,),
        in_specs=[pl.BlockSpec((1, BLOCK), lambda i: (0, i)), whole(table.shape)],
        out_specs=pl.BlockSpec((BLOCK, width), lambda i: (i, 0)),
        out_shape=jax.ShapeDtypeStruct((rows, width), bf16),
        compiler_params=params(),
        name="select_rows",
    )(idx, table)


def counts_kernel(adj_ref, out_ref):
    step = 16
    fanout = adj_ref.shape[1]
    width = out_ref.shape[1]
    lane = lax.broadcasted_iota(jnp.int32, (step, LANES), 1).astype(jnp.int16)
    one, zero = jnp.array(1, bf16), jnp.array(0, bf16)

    def body(r, carry):
        start = pl.multiple_of(r * step, step)
        rows = adj_ref[pl.ds(start, step), :]
        spread = [
            jnp.broadcast_to(rows[:, k : k + 1], (step, LANES)).astype(jnp.int16) for k in range(fanout)
        ]
        for j in range(width // LANES):
            here = lane + jnp.int16(LANES * j)
            acc = jnp.where(spread[0] == here, one, zero)
            for k in range(1, fanout):
                acc = acc + jnp.where(spread[k] == here, one, zero)
            out_ref[pl.ds(start, step), LANES * j : LANES * (j + 1)] = acc
        return carry

    lax.fori_loop(0, adj_ref.shape[0] // step, body, 0)


def counts(adjacency, width):
    rows, fanout = adjacency.shape
    block = min(rows, BLOCK)
    return pl.pallas_call(
        counts_kernel,
        grid=(rows // block,),
        in_specs=[pl.BlockSpec((block, fanout), lambda i: (i, 0))],
        out_specs=pl.BlockSpec((block, width), lambda i: (i, 0)),
        out_shape=jax.ShapeDtypeStruct((rows, width), bf16),
        compiler_params=params(),
        cost_estimate=pl.CostEstimate(
            flops=3 * fanout * rows * width, bytes_accessed=2 * rows * width, transcendentals=0
        ),
        name="neighbour_counts",
    )(adjacency)


def first_layer_kernel(
    slot_ref, arrived_ref, hot_ref, adj_ref, ws_ref, wn_ref, pre_ref, stat_ref, feat, acc, *, fanout
):
    i = pl.program_id(0)
    blocks = pl.num_programs(0) // 2

    @pl.when(i < blocks)
    def _():
        slot = slot_ref[...]
        pick = one_hot(slot, arrived_ref.shape[0])
        cold = jnp.dot(pick, arrived_ref[...], preferred_element_type=f32).astype(bf16)
        is_hot = row_to_lanes(slot) < 0
        reps = hot_ref.shape[1] // LANES
        cold = jnp.concatenate(
            [
                jnp.where(
                    is_hot,
                    hot_ref[:, LANES * j : LANES * (j + 1)].astype(f32),
                    cold[:, LANES * j : LANES * (j + 1)].astype(f32),
                ).astype(bf16)
                for j in range(reps)
            ],
            axis=1,
        )
        feat[pl.ds(pl.multiple_of(i * BLOCK, BLOCK), BLOCK), :] = cold

    @pl.when(i >= blocks)
    def _():
        b = i - blocks
        total = jnp.dot(adj_ref[...], feat[...], preferred_element_type=f32)
        mean = (total * (1.0 / fanout)).astype(bf16)
        own = feat[pl.ds(pl.multiple_of(b * BLOCK, BLOCK), BLOCK), :]
        pre = jnp.dot(own, ws_ref[...], preferred_element_type=f32) + jnp.dot(
            mean, wn_ref[...], preferred_element_type=f32
        )
        pre_ref[...] = pre
        grouped = pre.reshape(BLOCK // 8, 8, pre.shape[1])
        sums = jnp.sum(grouped, axis=0)
        squares = jnp.sum(grouped * grouped, axis=0)

        @pl.when(b == 0)
        def _():
            acc[0:8, :] = sums
            acc[8:16, :] = squares

        @pl.when(b > 0)
        def _():
            acc[0:8, :] += sums
            acc[8:16, :] += squares

        @pl.when(b == blocks - 1)
        def _():
            stat_ref[0:1, :] = jnp.sum(acc[0:8, :], axis=0, keepdims=True)
            stat_ref[1:2, :] = jnp.sum(acc[8:16, :], axis=0, keepdims=True)


def first_layer(slot, arrived, hot, adj, ws, wn, fanout):
    rows, width = adj.shape[0], hot.shape[1]
    hidden = ws.shape[1]
    blocks = rows // BLOCK
    first = lambda i: jnp.minimum(i, blocks - 1)
    second = lambda i: jnp.maximum(i - blocks, 0)
    return pl.pallas_call(
        functools.partial(first_layer_kernel, fanout=fanout),
        grid=(2 * blocks,),
        in_specs=[
            pl.BlockSpec((1, BLOCK), lambda i: (0, first(i))),
            whole(arrived.shape),
            pl.BlockSpec((BLOCK, width), lambda i: (first(i), 0)),
            pl.BlockSpec((BLOCK, rows), lambda i: (second(i), 0)),
            whole(ws.shape),
            whole(wn.shape),
        ],
        out_specs=[
            pl.BlockSpec((BLOCK, hidden), lambda i: (second(i), 0)),
            whole((2, hidden)),
        ],
        out_shape=[
            jax.ShapeDtypeStruct((rows, hidden), f32),
            jax.ShapeDtypeStruct((2, hidden), f32),
        ],
        scratch_shapes=[pltpu.VMEM((rows, width), bf16), pltpu.VMEM((16, hidden), f32)],
        compiler_params=params(),
        name="first_layer",
    )(slot, arrived, hot, adj, ws, wn)


def second_layer_kernel(
    pre_ref, stat_ref, gain_ref, shift_ref, send_ref, ws_ref, wn_ref, own_ref, neigh_ref, halo_ref, *, total_rows
):
    i = pl.program_id(0)
    mean = stat_ref[0:1, :] * (1.0 / total_rows)
    variance = stat_ref[1:2, :] * (1.0 / total_rows) - mean * mean
    scale = lax.rsqrt(variance + epsilon) * gain_ref[...]
    hidden = jnp.maximum((pre_ref[...] - mean) * scale + shift_ref[...], 0.0).astype(bf16)
    neigh = jnp.dot(hidden, wn_ref[...], preferred_element_type=f32).astype(bf16)
    neigh_ref[pl.ds(pl.multiple_of(i * BLOCK, BLOCK), BLOCK), :] = neigh

    @pl.when(i == 0)
    def _():
        own_ref[...] = jnp.dot(hidden, ws_ref[...], preferred_element_type=f32)

    @pl.when(i == pl.num_programs(0) - 1)
    def _():
        pick = one_hot(send_ref[...], neigh_ref.shape[0])
        halo_ref[...] = jnp.dot(pick, neigh_ref[...], preferred_element_type=f32).astype(bf16)


def second_layer(pre, stat, gain, shift, send, ws, wn, total_rows):
    rows, hidden = pre.shape
    classes = ws.shape[1]
    halo = send.shape[1]
    return pl.pallas_call(
        functools.partial(second_layer_kernel, total_rows=total_rows),
        grid=(rows // BLOCK,),
        in_specs=[
            pl.BlockSpec((BLOCK, hidden), lambda i: (i, 0)),
            whole((2, hidden)),
            whole((1, hidden)),
            whole((1, hidden)),
            whole((1, halo)),
            whole(ws.shape),
            whole(wn.shape),
        ],
        out_specs=[
            whole((BLOCK, classes)),
            whole((rows, classes)),
            whole((halo, classes)),
        ],
        out_shape=[
            jax.ShapeDtypeStruct((BLOCK, classes), f32),
            jax.ShapeDtypeStruct((rows, classes), bf16),
            jax.ShapeDtypeStruct((halo, classes), bf16),
        ],
        compiler_params=params(),
        name="second_layer",
    )(pre, stat, gain, shift, send, ws, wn)


def output_kernel(own_ref, adj_ref, neigh_ref, recv_ref, out_ref, *, fanout):
    rows = neigh_ref.shape[0]
    total = jnp.dot(adj_ref[:, :rows], neigh_ref[...], preferred_element_type=f32) + jnp.dot(
        adj_ref[:, rows:], recv_ref[...], preferred_element_type=f32
    )
    out_ref[...] = own_ref[...] + total * (1.0 / fanout)


def output(own, adj, neigh, recv, fanout):
    specs = [whole(a.shape) for a in (own, adj, neigh, recv)]
    return pl.pallas_call(
        functools.partial(output_kernel, fanout=fanout),
        grid=(1,),
        in_specs=specs,
        out_specs=whole(own.shape),
        out_shape=jax.ShapeDtypeStruct(own.shape, f32),
        compiler_params=params(),
        name="output_layer",
    )(own, adj, neigh, recv)


def local(
    hot_rows,
    cold_rows,
    hot_mask,
    hot_id,
    cold_owner,
    cold_pos,
    cold_send,
    adjacency_one,
    adjacency_two,
    halo_send,
    self_first,
    neigh_first,
    bn_gain,
    bn_shift,
    self_second,
    neigh_second,
):
    devices = lax.axis_size(HST_DEV)
    nodes = hot_mask.shape[0]
    targets = adjacency_two.shape[0]
    fan_one, fan_two = adjacency_one.shape[1], adjacency_two.shape[1]

    outgoing = select_rows(cold_send, cold_rows)
    slots = outgoing.shape[0] // devices
    arrived = lax.all_to_all(outgoing, HST_DEV, split_axis=0, concat_axis=0, tiled=True)

    hot_feat = hot_rows.at[hot_id].get(mode="promise_in_bounds")
    adj_one = counts(adjacency_one, nodes)
    adj_two = counts(adjacency_two, nodes + halo_send.shape[1])
    slot = jnp.where(hot_mask == 1, -1, cold_owner * slots + cold_pos)[None, :]

    pre, stat = first_layer(slot, arrived, hot_feat, adj_one, self_first, neigh_first, fan_one)
    stat = functools.reduce(lax.psum, HST_DEV, stat)
    own, neigh, halo = second_layer(
        pre,
        stat,
        bn_gain[None, :],
        bn_shift[None, :],
        halo_send,
        self_second,
        neigh_second,
        nodes * devices,
    )
    recv = lax.all_to_all(halo, DEV, split_axis=0, concat_axis=0, tiled=True)
    return output(own, adj_two, neigh, recv, fan_two)


def solution(mesh):
    torus = Mesh(mesh.devices.reshape(4, 2, 4, 4), ("hst_0", "hst_1", "dev_0", "dev_1"))
    split = P(HST_DEV)
    rows = P(HST_DEV, None)
    return jax.shard_map(
        local,
        mesh=torus,
        in_specs=(P(), rows, split, split, split, split, rows, rows, rows, rows, P(), P(), P(), P(), P(), P()),
        out_specs=rows,
        check_vma=False,
    )
```

```python
import functools

import jax
import jax.numpy as jnp
from jax import lax
from jax.experimental import pallas as pl
from jax.experimental.pallas import tpu as pltpu
from jax.sharding import Mesh
from jax.sharding import PartitionSpec as P

HST = ("hst_0", "hst_1")
DEV = ("dev_0", "dev_1")
HST_DEV = ("hst_0", "hst_1", "dev_0", "dev_1")

LANES = 128
BLOCK = 512
epsilon = 1e-05

f32 = jnp.float32
bf16 = jnp.bfloat16


def row_to_lanes(row):
    return jnp.transpose(jnp.broadcast_to(row, (LANES, row.shape[1])))


def one_hot(row, width):
    spread = row_to_lanes(row).astype(jnp.int16)
    lane = lax.broadcasted_iota(jnp.int32, spread.shape, 1).astype(jnp.int16)
    one, zero = jnp.array(1, bf16), jnp.array(0, bf16)
    tiles = [
        jnp.where(spread == lane + jnp.int16(LANES * j), one, zero) for j in range(width // LANES)
    ]
    return jnp.concatenate(tiles, axis=1)


VM = pl.BlockSpec(memory_space=pltpu.VMEM)
HBM = pl.BlockSpec(memory_space=pl.ANY)


def resident(array):
    return pltpu.with_memory_space_constraint(array, pltpu.VMEM)


def in_hbm(array):
    return pltpu.with_memory_space_constraint(array, pltpu.HBM)


def params(mib):
    return pltpu.CompilerParams(vmem_limit_bytes=mib * 2**20)


def whole(shape):
    return pl.BlockSpec(shape, lambda i: (0,) * len(shape))


def select_rows_kernel(idx_ref, table_ref, out_ref):
    hot = one_hot(idx_ref[...], table_ref.shape[0])
    out_ref[...] = jnp.dot(hot, table_ref[...], preferred_element_type=f32).astype(bf16)


def select_rows(idx, table):
    rows, width = idx.shape[1], table.shape[1]
    return pl.pallas_call(
        select_rows_kernel,
        grid=(rows // BLOCK,),
        in_specs=[pl.BlockSpec((1, BLOCK), lambda i: (0, i)), whole(table.shape)],
        out_specs=pl.BlockSpec((BLOCK, width), lambda i: (i, 0)),
        out_shape=pltpu.HBM((rows, width), bf16),
        compiler_params=params(24),
        name="select_rows",
    )(in_hbm(idx), in_hbm(table))


def count_neighbours(adj_ref, out_ref):
    step = 16
    group = 4
    fanout = adj_ref.shape[1]
    width = out_ref.shape[1]
    lane = lax.broadcasted_iota(jnp.int32, (step, LANES), 1).astype(jnp.int16)
    one, zero = jnp.array(1, bf16), jnp.array(0, bf16)

    def body(r, carry):
        for g in range(group):
            start = pl.multiple_of((r * group + g) * step, step)
            rows = adj_ref[pl.ds(start, step), :]
            spread = [
                jnp.broadcast_to(rows[:, k : k + 1], (step, LANES)).astype(jnp.int16) for k in range(fanout)
            ]
            for j in range(width // LANES):
                here = lane + jnp.int16(LANES * j)
                acc = jnp.where(spread[0] == here, one, zero)
                for k in range(1, fanout):
                    acc = acc + jnp.where(spread[k] == here, one, zero)
                out_ref[pl.ds(start, step), LANES * j : LANES * (j + 1)] = acc
        return carry

    lax.fori_loop(0, adj_ref.shape[0] // (step * group), body, 0)


def counts(adjacency, width):
    rows, fanout = adjacency.shape
    block = BLOCK // 2
    return pl.pallas_call(
        count_neighbours,
        grid=(rows // block,),
        in_specs=[pl.BlockSpec((block, fanout), lambda i: (i, 0))],
        out_specs=pl.BlockSpec((block, width), lambda i: (i, 0)),
        out_shape=pltpu.HBM((rows, width), bf16),
        compiler_params=params(24),
        cost_estimate=pl.CostEstimate(
            flops=3 * fanout * rows * width, bytes_accessed=2 * rows * width, transcendentals=0
        ),
        name="neighbour_counts",
    )(in_hbm(adjacency))


def first_layer_kernel(
    slot_ref, arrived_ref, hot_hbm, adj_hbm, ws_hbm, wn_hbm, pre_hbm, stat_ref,
    hot_ref, adj_ref, w_ref, pre_ref, hot_sem, adj_sem, ws_sem, wn_sem, pre_sem, both_ref, *, fanout
):
    rows, width = hot_ref.shape
    blocks = rows // BLOCK
    at = [pl.ds(b * BLOCK, BLOCK) for b in range(blocks)]
    hot_in = [pltpu.make_async_copy(hot_hbm.at[at[b]], hot_ref.at[at[b]], hot_sem.at[b]) for b in range(blocks)]
    adj_in = [pltpu.make_async_copy(adj_hbm.at[at[b]], adj_ref.at[at[b]], adj_sem.at[b]) for b in range(blocks)]
    ws_in = pltpu.make_async_copy(ws_hbm, w_ref.at[pl.ds(0, width)], ws_sem)
    wn_in = pltpu.make_async_copy(wn_hbm, w_ref.at[pl.ds(width, width)], wn_sem)
    pre_out = [pltpu.make_async_copy(pre_ref.at[b], pre_hbm.at[at[b]], pre_sem.at[b]) for b in range(blocks)]
    for copy in hot_in + [ws_in, wn_in] + adj_in:
        copy.start()
    for b in range(blocks):
        slot = slot_ref[:, at[b]]
        cold = jnp.dot(one_hot(slot, arrived_ref.shape[0]), arrived_ref[...], preferred_element_type=f32)
        is_hot = row_to_lanes(slot) < 0
        hot_in[b].wait()
        for j in range(width // LANES):
            lanes = slice(LANES * j, LANES * (j + 1))
            both_ref[at[b], lanes] = jnp.where(is_hot, hot_ref[at[b], lanes].astype(f32), cold[:, lanes]).astype(bf16)
    for b in range(blocks):
        adj_in[b].wait()
        total = jnp.dot(adj_ref[at[b], :], both_ref[:, :width], preferred_element_type=f32)
        both_ref[at[b], width:] = (total * (1.0 / fanout)).astype(bf16)
    ws_in.wait()
    wn_in.wait()
    sums = squares = 0
    for b in range(blocks):
        pre = jnp.dot(both_ref[at[b], :], w_ref[...], preferred_element_type=f32)
        pre_ref[b] = pre
        pre_out[b].start()
        grouped = pre.reshape(BLOCK // 8, 8, pre.shape[1])
        sums = sums + jnp.sum(grouped, axis=0)
        squares = squares + jnp.sum(grouped * grouped, axis=0)
    stat_ref[0:1, :] = jnp.sum(sums, axis=0, keepdims=True)
    stat_ref[1:2, :] = jnp.sum(squares, axis=0, keepdims=True)
    for b in range(blocks):
        pre_out[b].wait()


def first_layer(slot, arrived, hot, adj, ws, wn, fanout):
    rows, width = hot.shape
    hidden = ws.shape[1]
    blocks = rows // BLOCK
    return pl.pallas_call(
        functools.partial(first_layer_kernel, fanout=fanout),
        in_specs=[VM, VM, HBM, HBM, HBM, HBM],
        out_specs=[HBM, VM],
        out_shape=[
            pltpu.HBM((rows, hidden), f32),
            jax.ShapeDtypeStruct((2, hidden), f32),
        ],
        scratch_shapes=[
            pltpu.VMEM(hot.shape, bf16),
            pltpu.VMEM((rows, rows), bf16),
            pltpu.VMEM((2 * width, hidden), bf16),
            pltpu.VMEM((blocks, BLOCK, hidden), f32),
            pltpu.SemaphoreType.DMA((blocks,)),
            pltpu.SemaphoreType.DMA((blocks,)),
            pltpu.SemaphoreType.DMA,
            pltpu.SemaphoreType.DMA,
            pltpu.SemaphoreType.DMA((blocks,)),
            pltpu.VMEM((rows, 2 * width), bf16),
        ],
        compiler_params=params(48),
        name="first_layer",
    )(slot, resident(arrived), in_hbm(hot), in_hbm(adj), in_hbm(ws), in_hbm(wn))


def nt_dot(a, b):
    return lax.dot_general(a, b, (((1,), (1,)), ((), ())), preferred_element_type=f32)


def second_layer_kernel(
    pre_hbm, stat_ref, gain_ref, shift_ref, send_ref, ws_hbm, wn_hbm, own_hbm, neigh_hbm, halo_ref,
    pre_ref, ws_ref, wn_ref, own_ref, neigh_ref, pre_sem, ws_sem, wn_sem, own_sem, neigh_sem, *, total_rows
):
    blocks = pre_ref.shape[0] // BLOCK
    at = [pl.ds(b * BLOCK, BLOCK) for b in range(blocks)]
    pre_in = [pltpu.make_async_copy(pre_hbm.at[at[b]], pre_ref.at[at[b]], pre_sem.at[b]) for b in range(blocks)]
    ws_in = pltpu.make_async_copy(ws_hbm, ws_ref, ws_sem)
    wn_in = pltpu.make_async_copy(wn_hbm, wn_ref, wn_sem)
    own_out = pltpu.make_async_copy(own_ref, own_hbm, own_sem)
    neigh_out = pltpu.make_async_copy(neigh_ref, neigh_hbm, neigh_sem)
    for copy in [pre_in[0], wn_in, ws_in] + pre_in[1:]:
        copy.start()
    mean = stat_ref[0:1, :] * (1.0 / total_rows)
    variance = stat_ref[1:2, :] * (1.0 / total_rows) - mean * mean
    scale = lax.rsqrt(variance + epsilon) * gain_ref[...]
    shift = shift_ref[...]
    for b in range(blocks):
        pre_in[b].wait()
        hidden = jnp.maximum((pre_ref[at[b], :] - mean) * scale + shift, 0.0).astype(bf16)
        if b == 0:
            wn_in.wait()
            ws_in.wait()
            own_ref[...] = nt_dot(hidden, ws_ref[...])
            own_out.start()
        neigh_ref[at[b], :] = nt_dot(hidden, wn_ref[...]).astype(bf16)
    neigh_out.start()
    pick = one_hot(send_ref[...], neigh_ref.shape[0])
    halo_ref[...] = jnp.dot(pick, neigh_ref[...], preferred_element_type=f32).astype(bf16)
    own_out.wait()
    neigh_out.wait()


def second_layer(pre, stat, gain, shift, send, ws, wn, total_rows):
    rows, hidden = pre.shape
    classes = ws.shape[0]
    halo = send.shape[1]
    dma = pltpu.SemaphoreType.DMA
    return pl.pallas_call(
        functools.partial(second_layer_kernel, total_rows=total_rows),
        in_specs=[HBM, VM, VM, VM, VM, HBM, HBM],
        out_specs=[HBM, HBM, VM],
        out_shape=[
            pltpu.HBM((BLOCK, classes), f32),
            pltpu.HBM((rows, classes), bf16),
            jax.ShapeDtypeStruct((halo, classes), bf16),
        ],
        scratch_shapes=[
            pltpu.VMEM(pre.shape, f32),
            pltpu.VMEM(ws.shape, bf16),
            pltpu.VMEM(wn.shape, bf16),
            pltpu.VMEM((BLOCK, classes), f32),
            pltpu.VMEM((rows, classes), bf16),
            dma((rows // BLOCK,)),
            dma,
            dma,
            dma,
            dma,
        ],
        compiler_params=params(32),
        name="second_layer",
    )(in_hbm(pre), stat, gain, shift, send, in_hbm(ws), in_hbm(wn))


def targets_kernel(adj_ref, own_hbm, neigh_hbm, part_ref, far_ref, count_ref, own_ref, neigh_ref, own_sem, neigh_sem):
    rows = neigh_ref.shape[0]
    own_in = pltpu.make_async_copy(own_hbm, own_ref, own_sem)
    neigh_in = pltpu.make_async_copy(neigh_hbm, neigh_ref, neigh_sem)
    own_in.start()
    neigh_in.start()
    count_neighbours(adj_ref, count_ref)
    own_in.wait()
    neigh_in.wait()
    total = jnp.dot(count_ref[:, :rows], neigh_ref[...], preferred_element_type=f32)
    part_ref[...] = own_ref[...] + total * (1.0 / adj_ref.shape[1])
    far_ref[...] = count_ref[:, rows:]


def targets_layer(adj, own, neigh, halo):
    count, rows = adj.shape[0], neigh.shape[0]
    return pl.pallas_call(
        targets_kernel,
        in_specs=[VM, HBM, HBM],
        out_specs=[VM, VM],
        out_shape=[jax.ShapeDtypeStruct(own.shape, f32), jax.ShapeDtypeStruct((count, halo), bf16)],
        scratch_shapes=[
            pltpu.VMEM((count, rows + halo), bf16),
            pltpu.VMEM(own.shape, f32),
            pltpu.VMEM(neigh.shape, bf16),
            pltpu.SemaphoreType.DMA,
            pltpu.SemaphoreType.DMA,
        ],
        compiler_params=params(16),
        cost_estimate=pl.CostEstimate(
            flops=3 * adj.shape[1] * count * (rows + halo), bytes_accessed=2 * count * rows, transcendentals=0
        ),
        name="targets_layer",
    )(adj, in_hbm(own), in_hbm(neigh))


def output_kernel(part_ref, far_ref, recv_ref, out_ref, *, fanout):
    total = jnp.dot(far_ref[...], recv_ref[...], preferred_element_type=f32)
    out_ref[...] = jnp.transpose(part_ref[...] + total * (1.0 / fanout))


def output(part, far, recv, fanout):
    return pl.pallas_call(
        functools.partial(output_kernel, fanout=fanout),
        in_specs=[VM] * 3,
        out_specs=VM,
        out_shape=jax.ShapeDtypeStruct(part.shape[::-1], f32),
        compiler_params=params(16),
        name="output_layer",
    )(part, far, recv).T


def sum_over(array, axes):
    copies = jnp.broadcast_to(array[None], (lax.axis_size(axes),) + array.shape)
    return jnp.sum(lax.all_to_all(copies, axes, split_axis=0, concat_axis=0, tiled=True), axis=0)


def local(
    hot_rows,
    cold_rows,
    hot_mask,
    hot_id,
    cold_owner,
    cold_pos,
    cold_send,
    adjacency_one,
    adjacency_two,
    halo_send,
    self_first,
    neigh_first,
    bn_gain,
    bn_shift,
    self_second,
    neigh_second,
):
    devices = lax.axis_size(HST_DEV)
    nodes = hot_mask.shape[0]
    fan_one, fan_two = adjacency_one.shape[1], adjacency_two.shape[1]

    outgoing = select_rows(cold_send, cold_rows)
    slots = outgoing.shape[0] // devices
    arrived = lax.all_to_all(outgoing, HST_DEV, split_axis=0, concat_axis=0, tiled=True)

    hot_feat = hot_rows.at[hot_id].get(mode="promise_in_bounds")
    adj_one = counts(adjacency_one, nodes)
    slot = jnp.where(hot_mask == 1, -1, cold_owner * slots + cold_pos)[None, :]

    pre, stat = first_layer(slot, arrived, hot_feat, adj_one, self_first, neigh_first, fan_one)
    stat = sum_over(sum_over(stat, HST), DEV)
    own, neigh, halo = second_layer(
        pre,
        stat,
        bn_gain[None, :],
        bn_shift[None, :],
        halo_send,
        self_second.T,
        neigh_second.T,
        nodes * devices,
    )
    recv = lax.all_to_all(halo, DEV, split_axis=0, concat_axis=0, tiled=True)
    part, far = targets_layer(adjacency_two, own, neigh, halo_send.shape[1])
    return output(part, far, recv, fan_two)


def solution(mesh):
    torus = Mesh(mesh.devices.reshape(4, 2, 4, 4), ("hst_0", "hst_1", "dev_0", "dev_1"))
    split = P(HST_DEV)
    rows = P(HST_DEV, None)
    return jax.shard_map(
        local,
        mesh=torus,
        in_specs=(P(), rows, split, split, split, split, rows, rows, rows, rows, P(), P(), P(), P(), P(), P()),
        out_specs=rows,
        check_vma=False,
    )
```

```python
import functools

import jax
import jax.numpy as jnp
from jax import lax
from jax.experimental import pallas as pl
from jax.experimental.pallas import tpu as pltpu
from jax.sharding import Mesh
from jax.sharding import PartitionSpec as P

HST = ("hst_0", "hst_1")
DEV = ("dev_0", "dev_1")
HST_DEV = ("hst_0", "hst_1", "dev_0", "dev_1")

LANES = 128
BLOCK = 512
epsilon = 1e-05

f32 = jnp.float32
bf16 = jnp.bfloat16


def row_to_lanes(row):
    return jnp.transpose(jnp.broadcast_to(row, (LANES, row.shape[1]))).astype(jnp.int16)


def one_hot(spread, width):
    lane = lax.broadcasted_iota(jnp.int32, spread.shape, 1).astype(jnp.int16)
    one, zero = jnp.array(1, bf16), jnp.array(0, bf16)
    tiles = [
        jnp.where(spread == lane + jnp.int16(LANES * j), one, zero) for j in range(width // LANES)
    ]
    return jnp.concatenate(tiles, axis=1)


VM = pl.BlockSpec(memory_space=pltpu.VMEM)
HBM = pl.BlockSpec(memory_space=pl.ANY)


def resident(array):
    return pltpu.with_memory_space_constraint(array, pltpu.VMEM)


def in_hbm(array):
    return pltpu.with_memory_space_constraint(array, pltpu.HBM)


def params(mib):
    return pltpu.CompilerParams(vmem_limit_bytes=mib * 2**20)


def whole(shape):
    return pl.BlockSpec(shape, lambda i: (0,) * len(shape))


def select_rows_kernel(idx_ref, table_ref, out_ref):
    hot = one_hot(row_to_lanes(idx_ref[...]), table_ref.shape[0])
    out_ref[...] = jnp.dot(hot, table_ref[...], preferred_element_type=f32).astype(bf16)


def select_rows(idx, table):
    rows, width = idx.shape[1], table.shape[1]
    return pl.pallas_call(
        select_rows_kernel,
        grid=(rows // BLOCK,),
        in_specs=[pl.BlockSpec((1, BLOCK), lambda i: (0, i)), whole(table.shape)],
        out_specs=pl.BlockSpec((BLOCK, width), lambda i: (i, 0)),
        out_shape=pltpu.HBM((rows, width), bf16),
        compiler_params=params(24),
        name="select_rows",
    )(in_hbm(idx), in_hbm(table))


def count_neighbours(adj_ref, out_ref):
    step = 16
    group = 8
    fanout = adj_ref.shape[1]
    width = out_ref.shape[1]
    lane = lax.broadcasted_iota(jnp.int32, (step, LANES), 1).astype(jnp.int16)
    one, zero = jnp.array(1, bf16), jnp.array(0, bf16)

    def body(r, carry):
        for g in range(group):
            start = pl.multiple_of((r * group + g) * step, step)
            rows = adj_ref[pl.ds(start, step), :]
            spread = [
                jnp.broadcast_to(rows[:, k : k + 1], (step, LANES)).astype(jnp.int16) for k in range(fanout)
            ]
            for j in range(width // LANES):
                here = lane + jnp.int16(LANES * j)
                acc = jnp.where(spread[0] == here, one, zero)
                for k in range(1, fanout):
                    acc = acc + jnp.where(spread[k] == here, one, zero)
                out_ref[pl.ds(start, step), LANES * j : LANES * (j + 1)] = acc
        return carry

    lax.fori_loop(0, adj_ref.shape[0] // (step * group), body, 0)


def counts(adjacency, width):
    rows, fanout = adjacency.shape
    block = BLOCK // 2
    return pl.pallas_call(
        count_neighbours,
        grid=(rows // block,),
        in_specs=[pl.BlockSpec((block, fanout), lambda i: (i, 0))],
        out_specs=pl.BlockSpec((block, width), lambda i: (i, 0)),
        out_shape=pltpu.HBM((rows, width), bf16),
        compiler_params=params(24),
        cost_estimate=pl.CostEstimate(
            flops=3 * fanout * rows * width, bytes_accessed=2 * rows * width, transcendentals=0
        ),
        name="neighbour_counts",
    )(in_hbm(adjacency))


def first_layer_kernel(
    slot_ref, arrived_ref, hot_hbm, adj_hbm, ws_hbm, wn_hbm, pre_hbm, stat_ref,
    hot_ref, adj_ref, w_ref, pre_ref, hot_sem, adj_sem, ws_sem, wn_sem, pre_sem, both_ref, *, fanout
):
    rows, width = hot_ref.shape
    blocks = rows // BLOCK
    at = [pl.ds(b * BLOCK, BLOCK) for b in range(blocks)]
    out = at[:-1] + [pl.ds(rows - BLOCK, BLOCK // 2), pl.ds(rows - BLOCK // 2, BLOCK // 2)]
    hot_in = pltpu.make_async_copy(hot_hbm, hot_ref, hot_sem)
    adj_in = pltpu.make_async_copy(adj_hbm, adj_ref, adj_sem)
    ws_in = pltpu.make_async_copy(ws_hbm, w_ref.at[pl.ds(0, width)], ws_sem)
    wn_in = pltpu.make_async_copy(wn_hbm, w_ref.at[pl.ds(width, width)], wn_sem)
    pre_out = [pltpu.make_async_copy(pre_ref.at[out[b]], pre_hbm.at[out[b]], pre_sem.at[b]) for b in range(len(out))]
    hot_in.start()
    for b in range(blocks):
        spread = row_to_lanes(slot_ref[:, at[b]])
        cold = jnp.dot(one_hot(spread, arrived_ref.shape[0]), arrived_ref[...], preferred_element_type=f32).astype(bf16)
        if b == 0:
            hot_in.wait()
            for copy in (adj_in, ws_in, wn_in):
                copy.start()
        for j in range(width // LANES):
            lanes = slice(LANES * j, LANES * (j + 1))
            both_ref[at[b], lanes] = jnp.where(spread < jnp.int16(0), hot_ref[at[b], lanes], cold[:, lanes])
    adj_in.wait()
    ws_in.wait()
    wn_in.wait()
    for b in range(blocks):
        total = jnp.dot(adj_ref[at[b], :], both_ref[:, :width], preferred_element_type=f32)
        both_ref[at[b], width:] = (total * (1.0 / fanout)).astype(bf16)
    sums = squares = 0
    for b in range(len(out)):
        pre = jnp.dot(both_ref[out[b], :], w_ref[...], preferred_element_type=f32)
        pre_ref[out[b], :] = pre
        pre_out[b].start()
        grouped = pre.reshape(pre.shape[0] // 8, 8, pre.shape[1])
        sums = sums + jnp.sum(grouped, axis=0)
        squares = squares + jnp.sum(grouped * grouped, axis=0)
    stat_ref[0:1, :] = jnp.sum(sums, axis=0, keepdims=True)
    stat_ref[1:2, :] = jnp.sum(squares, axis=0, keepdims=True)
    for copy in pre_out:
        copy.wait()


def first_layer(slot, arrived, hot, adj, ws, wn, fanout):
    rows, width = hot.shape
    hidden = ws.shape[1]
    blocks = rows // BLOCK
    return pl.pallas_call(
        functools.partial(first_layer_kernel, fanout=fanout),
        in_specs=[VM, VM, HBM, HBM, HBM, HBM],
        out_specs=[HBM, VM],
        out_shape=[
            pltpu.HBM((rows, hidden), f32),
            jax.ShapeDtypeStruct((2, hidden), f32),
        ],
        scratch_shapes=[
            pltpu.VMEM(hot.shape, bf16),
            pltpu.VMEM((rows, rows), bf16),
            pltpu.VMEM((2 * width, hidden), bf16),
            pltpu.VMEM((rows, hidden), f32),
            pltpu.SemaphoreType.DMA,
            pltpu.SemaphoreType.DMA,
            pltpu.SemaphoreType.DMA,
            pltpu.SemaphoreType.DMA,
            pltpu.SemaphoreType.DMA((blocks + 1,)),
            pltpu.VMEM((rows, 2 * width), bf16),
        ],
        compiler_params=params(48),
        name="first_layer",
    )(slot, resident(arrived), in_hbm(hot), in_hbm(adj), in_hbm(ws), in_hbm(wn))


def nt_dot(a, b):
    return lax.dot_general(a, b, (((1,), (1,)), ((), ())), preferred_element_type=f32)


def second_layer_kernel(
    pre_hbm, stat_ref, gain_ref, shift_ref, send_ref, ws_hbm, wn_hbm, own_hbm, neigh_hbm, halo_ref,
    pre_ref, ws_ref, wn_ref, own_ref, neigh_ref, pre_sem, ws_sem, wn_sem, own_sem, neigh_sem, *, total_rows
):
    blocks = pre_ref.shape[0] // BLOCK
    at = [pl.ds(b * BLOCK, BLOCK) for b in range(blocks)]
    pre_in = [pltpu.make_async_copy(pre_hbm.at[at[b]], pre_ref.at[at[b]], pre_sem.at[b]) for b in range(blocks)]
    ws_in = pltpu.make_async_copy(ws_hbm, ws_ref, ws_sem)
    wn_in = pltpu.make_async_copy(wn_hbm, wn_ref, wn_sem)
    own_out = pltpu.make_async_copy(own_ref, own_hbm, own_sem)
    neigh_out = pltpu.make_async_copy(neigh_ref, neigh_hbm, neigh_sem)
    for copy in [pre_in[0], wn_in, ws_in] + pre_in[1:]:
        copy.start()
    mean = stat_ref[0:1, :] * (1.0 / total_rows)
    variance = stat_ref[1:2, :] * (1.0 / total_rows) - mean * mean
    scale = lax.rsqrt(variance + epsilon) * gain_ref[...]
    shift = shift_ref[...]
    for b in range(blocks):
        pre_in[b].wait()
        hidden = jnp.maximum((pre_ref[at[b], :] - mean) * scale + shift, 0.0).astype(bf16)
        if b == 0:
            wn_in.wait()
            ws_in.wait()
            own_ref[...] = nt_dot(hidden, ws_ref[...])
            own_out.start()
        neigh_ref[at[b], :] = nt_dot(hidden, wn_ref[...]).astype(bf16)
    neigh_out.start()
    pick = one_hot(row_to_lanes(send_ref[...]), neigh_ref.shape[0])
    halo_ref[...] = jnp.dot(pick, neigh_ref[...], preferred_element_type=f32).astype(bf16)
    own_out.wait()
    neigh_out.wait()


def second_layer(pre, stat, gain, shift, send, ws, wn, total_rows):
    rows, hidden = pre.shape
    classes = ws.shape[0]
    halo = send.shape[1]
    dma = pltpu.SemaphoreType.DMA
    return pl.pallas_call(
        functools.partial(second_layer_kernel, total_rows=total_rows),
        in_specs=[HBM, VM, VM, VM, VM, HBM, HBM],
        out_specs=[HBM, HBM, VM],
        out_shape=[
            pltpu.HBM((BLOCK, classes), f32),
            pltpu.HBM((rows, classes), bf16),
            jax.ShapeDtypeStruct((halo, classes), bf16),
        ],
        scratch_shapes=[
            pltpu.VMEM(pre.shape, f32),
            pltpu.VMEM(ws.shape, bf16),
            pltpu.VMEM(wn.shape, bf16),
            pltpu.VMEM((BLOCK, classes), f32),
            pltpu.VMEM((rows, classes), bf16),
            dma((rows // BLOCK,)),
            dma,
            dma,
            dma,
            dma,
        ],
        compiler_params=params(32),
        name="second_layer",
    )(in_hbm(pre), stat, gain, shift, send, in_hbm(ws), in_hbm(wn))


def targets_kernel(adj_ref, own_hbm, neigh_hbm, part_ref, far_ref, count_ref, own_ref, neigh_ref, own_sem, neigh_sem):
    rows = neigh_ref.shape[0]
    own_in = pltpu.make_async_copy(own_hbm, own_ref, own_sem)
    neigh_in = pltpu.make_async_copy(neigh_hbm, neigh_ref, neigh_sem)
    own_in.start()
    neigh_in.start()
    count_neighbours(adj_ref, count_ref)
    own_in.wait()
    neigh_in.wait()
    total = jnp.dot(count_ref[:, :rows], neigh_ref[...], preferred_element_type=f32)
    part_ref[...] = own_ref[...] + total * (1.0 / adj_ref.shape[1])
    far_ref[...] = count_ref[:, rows:]


def targets_layer(adj, own, neigh, halo):
    count, rows = adj.shape[0], neigh.shape[0]
    return pl.pallas_call(
        targets_kernel,
        in_specs=[VM, HBM, HBM],
        out_specs=[VM, VM],
        out_shape=[jax.ShapeDtypeStruct(own.shape, f32), jax.ShapeDtypeStruct((count, halo), bf16)],
        scratch_shapes=[
            pltpu.VMEM((count, rows + halo), bf16),
            pltpu.VMEM(own.shape, f32),
            pltpu.VMEM(neigh.shape, bf16),
            pltpu.SemaphoreType.DMA,
            pltpu.SemaphoreType.DMA,
        ],
        compiler_params=params(16),
        cost_estimate=pl.CostEstimate(
            flops=3 * adj.shape[1] * count * (rows + halo), bytes_accessed=2 * count * rows, transcendentals=0
        ),
        name="targets_layer",
    )(adj, in_hbm(own), in_hbm(neigh))


def output_kernel(part_ref, far_ref, recv_ref, out_ref, *, fanout):
    total = jnp.dot(far_ref[...], recv_ref[...], preferred_element_type=f32)
    out_ref[...] = jnp.transpose(part_ref[...] + total * (1.0 / fanout))


def output(part, far, recv, fanout):
    return pl.pallas_call(
        functools.partial(output_kernel, fanout=fanout),
        in_specs=[VM] * 3,
        out_specs=VM,
        out_shape=jax.ShapeDtypeStruct(part.shape[::-1], f32),
        compiler_params=params(16),
        name="output_layer",
    )(part, far, recv).T


def sum_over(array, axes):
    copies = jnp.broadcast_to(array[None], (lax.axis_size(axes),) + array.shape)
    return jnp.sum(lax.all_to_all(copies, axes, split_axis=0, concat_axis=0, tiled=True), axis=0)


def local(
    hot_rows,
    cold_rows,
    hot_mask,
    hot_id,
    cold_owner,
    cold_pos,
    cold_send,
    adjacency_one,
    adjacency_two,
    halo_send,
    self_first,
    neigh_first,
    bn_gain,
    bn_shift,
    self_second,
    neigh_second,
):
    devices = lax.axis_size(HST_DEV)
    nodes = hot_mask.shape[0]
    fan_one, fan_two = adjacency_one.shape[1], adjacency_two.shape[1]

    outgoing = select_rows(cold_send, cold_rows)
    slots = outgoing.shape[0] // devices
    arrived = lax.all_to_all(outgoing, HST_DEV, split_axis=0, concat_axis=0, tiled=True)

    hot_feat = hot_rows.at[hot_id].get(mode="promise_in_bounds")
    adj_one = counts(adjacency_one, nodes)
    slot = jnp.where(hot_mask == 1, -1, cold_owner * slots + cold_pos)[None, :]

    pre, stat = first_layer(slot, arrived, hot_feat, adj_one, self_first, neigh_first, fan_one)
    stat = sum_over(sum_over(stat, HST), DEV)
    own, neigh, halo = second_layer(
        pre,
        stat,
        bn_gain[None, :],
        bn_shift[None, :],
        halo_send,
        self_second.T,
        neigh_second.T,
        nodes * devices,
    )
    recv = lax.all_to_all(halo, DEV, split_axis=0, concat_axis=0, tiled=True)
    part, far = targets_layer(adjacency_two, own, neigh, halo_send.shape[1])
    return output(part, far, recv, fan_two)


def solution(mesh):
    torus = Mesh(mesh.devices.reshape(4, 2, 4, 4), ("hst_0", "hst_1", "dev_0", "dev_1"))
    split = P(HST_DEV)
    rows = P(HST_DEV, None)
    return jax.shard_map(
        local,
        mesh=torus,
        in_specs=(P(), rows, split, split, split, split, rows, rows, rows, rows, P(), P(), P(), P(), P(), P()),
        out_specs=rows,
        check_vma=False,
    )
```

```python
import functools

import jax
import jax.numpy as jnp
from jax import lax
from jax.experimental import pallas as pl
from jax.experimental.pallas import tpu as pltpu
from jax.sharding import Mesh
from jax.sharding import PartitionSpec as P

HST = ("hst_0", "hst_1")
DEV = ("dev_0", "dev_1")
HST_DEV = ("hst_0", "hst_1", "dev_0", "dev_1")

LANES = 128
BLOCK = 512
epsilon = 1e-05

f32 = jnp.float32
bf16 = jnp.bfloat16


def row_to_lanes(row):
    return jnp.transpose(jnp.broadcast_to(row, (LANES, row.shape[1]))).astype(jnp.int16)


def one_hot(spread, width):
    lane = lax.broadcasted_iota(jnp.int32, spread.shape, 1).astype(jnp.int16)
    one, zero = jnp.array(1, bf16), jnp.array(0, bf16)
    tiles = [
        jnp.where(spread == lane + jnp.int16(LANES * j), one, zero) for j in range(width // LANES)
    ]
    return jnp.concatenate(tiles, axis=1)


VM = pl.BlockSpec(memory_space=pltpu.VMEM)
HBM = pl.BlockSpec(memory_space=pl.ANY)


def resident(array):
    return pltpu.with_memory_space_constraint(array, pltpu.VMEM)


def in_hbm(array):
    return pltpu.with_memory_space_constraint(array, pltpu.HBM)


def params(mib):
    return pltpu.CompilerParams(vmem_limit_bytes=mib * 2**20)


def whole(shape):
    return pl.BlockSpec(shape, lambda i: (0,) * len(shape))


def select_rows_kernel(idx_hbm, table_hbm, out_hbm, idx_ref, table_ref, out_ref, idx_sem, table_sem, out_sem):
    blocks = out_ref.shape[0] // BLOCK
    at = [pl.ds(b * BLOCK, BLOCK) for b in range(blocks)]
    idx_in = pltpu.make_async_copy(idx_hbm, idx_ref, idx_sem)
    table_in = pltpu.make_async_copy(table_hbm, table_ref, table_sem)
    copies = [pltpu.make_async_copy(out_ref.at[at[b]], out_hbm.at[at[b]], out_sem.at[b]) for b in range(blocks)]
    idx_in.start()
    table_in.start()
    idx_in.wait()
    spread = [row_to_lanes(idx_ref[:, at[b]]) for b in range(blocks)]
    table_in.wait()
    for b in range(blocks):
        pick = one_hot(spread[b], table_ref.shape[0])
        out_ref[at[b], :] = jnp.dot(pick, table_ref[...], preferred_element_type=f32).astype(bf16)
        copies[b].start()
    for copy in copies:
        copy.wait()


def select_rows(idx, table):
    rows, width = idx.shape[1], table.shape[1]
    return pl.pallas_call(
        select_rows_kernel,
        in_specs=[HBM, HBM],
        out_specs=HBM,
        out_shape=pltpu.HBM((rows, width), bf16),
        scratch_shapes=[
            pltpu.VMEM(idx.shape, jnp.int32),
            pltpu.VMEM(table.shape, bf16),
            pltpu.VMEM((rows, width), bf16),
            pltpu.SemaphoreType.DMA,
            pltpu.SemaphoreType.DMA,
            pltpu.SemaphoreType.DMA((rows // BLOCK,)),
        ],
        compiler_params=params(24),
        name="select_rows",
    )(in_hbm(idx), in_hbm(table))


def count_neighbours(adj_ref, out_ref):
    step = 16
    group = 8
    fanout = adj_ref.shape[1]
    width = out_ref.shape[1]
    lane = lax.broadcasted_iota(jnp.int32, (step, LANES), 1).astype(jnp.int16)
    one, zero = jnp.array(1, bf16), jnp.array(0, bf16)

    def body(r, carry):
        for g in range(group):
            start = pl.multiple_of((r * group + g) * step, step)
            rows = adj_ref[pl.ds(start, step), :]
            spread = [
                jnp.broadcast_to(rows[:, k : k + 1], (step, LANES)).astype(jnp.int16) for k in range(fanout)
            ]
            for j in range(width // LANES):
                here = lane + jnp.int16(LANES * j)
                acc = jnp.where(spread[0] == here, one, zero)
                for k in range(1, fanout):
                    acc = acc + jnp.where(spread[k] == here, one, zero)
                out_ref[pl.ds(start, step), LANES * j : LANES * (j + 1)] = acc
        return carry

    lax.fori_loop(0, adj_ref.shape[0] // (step * group), body, 0)


def counts(adjacency, width):
    rows, fanout = adjacency.shape
    block = BLOCK // 2
    return pl.pallas_call(
        count_neighbours,
        grid=(rows // block,),
        in_specs=[pl.BlockSpec((block, fanout), lambda i: (i, 0))],
        out_specs=pl.BlockSpec((block, width), lambda i: (i, 0)),
        out_shape=pltpu.HBM((rows, width), bf16),
        compiler_params=params(24),
        cost_estimate=pl.CostEstimate(
            flops=3 * fanout * rows * width, bytes_accessed=2 * rows * width, transcendentals=0
        ),
        name="neighbour_counts",
    )(in_hbm(adjacency))


def first_layer_kernel(
    slot_ref, arrived_ref, hot_hbm, adj_hbm, ws_hbm, wn_hbm, pre_hbm, stat_ref,
    hot_ref, adj_ref, w_ref, pre_ref, hot_sem, adj_sem, ws_sem, wn_sem, pre_sem, both_ref, *, fanout
):
    rows, width = hot_ref.shape
    blocks = rows // BLOCK
    at = [pl.ds(b * BLOCK, BLOCK) for b in range(blocks)]
    out = at[:-1] + [pl.ds(rows - BLOCK, BLOCK // 2), pl.ds(rows - BLOCK // 2, BLOCK // 2)]
    hot_in = pltpu.make_async_copy(hot_hbm, hot_ref, hot_sem)
    adj_in = pltpu.make_async_copy(adj_hbm, adj_ref, adj_sem)
    ws_in = pltpu.make_async_copy(ws_hbm, w_ref.at[pl.ds(0, width)], ws_sem)
    wn_in = pltpu.make_async_copy(wn_hbm, w_ref.at[pl.ds(width, width)], wn_sem)
    pre_out = [pltpu.make_async_copy(pre_ref.at[out[b]], pre_hbm.at[out[b]], pre_sem.at[b]) for b in range(len(out))]
    hot_in.start()
    for b in range(blocks):
        spread = row_to_lanes(slot_ref[:, at[b]])
        cold = jnp.dot(one_hot(spread, arrived_ref.shape[0]), arrived_ref[...], preferred_element_type=f32).astype(bf16)
        if b == 0:
            hot_in.wait()
            for copy in (adj_in, ws_in, wn_in):
                copy.start()
        for j in range(width // LANES):
            lanes = slice(LANES * j, LANES * (j + 1))
            both_ref[at[b], lanes] = jnp.where(spread < jnp.int16(0), hot_ref[at[b], lanes], cold[:, lanes])
    adj_in.wait()
    ws_in.wait()
    wn_in.wait()
    for b in range(blocks):
        total = jnp.dot(adj_ref[at[b], :], both_ref[:, :width], preferred_element_type=f32)
        both_ref[at[b], width:] = (total * (1.0 / fanout)).astype(bf16)
    sums = squares = 0
    for b in range(len(out)):
        pre = jnp.dot(both_ref[out[b], :], w_ref[...], preferred_element_type=f32)
        pre_ref[out[b], :] = pre
        pre_out[b].start()
        grouped = pre.reshape(pre.shape[0] // 8, 8, pre.shape[1])
        sums = sums + jnp.sum(grouped, axis=0)
        squares = squares + jnp.sum(grouped * grouped, axis=0)
    stat_ref[0:1, :] = jnp.sum(sums, axis=0, keepdims=True)
    stat_ref[1:2, :] = jnp.sum(squares, axis=0, keepdims=True)
    for copy in pre_out:
        copy.wait()


def first_layer(slot, arrived, hot, adj, ws, wn, fanout):
    rows, width = hot.shape
    hidden = ws.shape[1]
    blocks = rows // BLOCK
    return pl.pallas_call(
        functools.partial(first_layer_kernel, fanout=fanout),
        in_specs=[VM, VM, HBM, HBM, HBM, HBM],
        out_specs=[HBM, VM],
        out_shape=[
            pltpu.HBM((rows, hidden), f32),
            jax.ShapeDtypeStruct((2, hidden), f32),
        ],
        scratch_shapes=[
            pltpu.VMEM(hot.shape, bf16),
            pltpu.VMEM((rows, rows), bf16),
            pltpu.VMEM((2 * width, hidden), bf16),
            pltpu.VMEM((rows, hidden), f32),
            pltpu.SemaphoreType.DMA,
            pltpu.SemaphoreType.DMA,
            pltpu.SemaphoreType.DMA,
            pltpu.SemaphoreType.DMA,
            pltpu.SemaphoreType.DMA((blocks + 1,)),
            pltpu.VMEM((rows, 2 * width), bf16),
        ],
        compiler_params=params(48),
        name="first_layer",
    )(slot, resident(arrived), in_hbm(hot), in_hbm(adj), in_hbm(ws), in_hbm(wn))


def nt_dot(a, b):
    return lax.dot_general(a, b, (((1,), (1,)), ((), ())), preferred_element_type=f32)


def second_layer_kernel(
    pre_hbm, stat_ref, gain_ref, shift_ref, send_ref, ws_hbm, wn_hbm, own_hbm, neigh_hbm, halo_ref,
    pre_ref, ws_ref, wn_ref, own_ref, neigh_ref, pre_sem, ws_sem, wn_sem, own_sem, neigh_sem, *, total_rows
):
    step = BLOCK // 2
    at = [pl.ds(start, step) for start in range(0, pre_ref.shape[0], step)]
    pre_in = [pltpu.make_async_copy(pre_hbm.at[rows], pre_ref.at[rows], pre_sem.at[b]) for b, rows in enumerate(at)]
    ws_in = pltpu.make_async_copy(ws_hbm, ws_ref, ws_sem)
    wn_in = pltpu.make_async_copy(wn_hbm, wn_ref, wn_sem)
    own_out = pltpu.make_async_copy(own_ref, own_hbm, own_sem)
    neigh_out = pltpu.make_async_copy(neigh_ref, neigh_hbm, neigh_sem)
    for copy in [wn_in] + pre_in[:3] + [ws_in]:
        copy.start()
    spread = row_to_lanes(send_ref[...])
    mean = stat_ref[0:1, :] * (1.0 / total_rows)
    variance = stat_ref[1:2, :] * (1.0 / total_rows) - mean * mean
    scale = lax.rsqrt(variance + epsilon) * gain_ref[...]
    shift = shift_ref[...]
    for b, rows in enumerate(at):
        pre_in[b].wait()
        if b + 3 < len(at):
            pre_in[b + 3].start()
        hidden = jnp.maximum((pre_ref[rows, :] - mean) * scale + shift, 0.0).astype(bf16)
        if b == 0:
            wn_in.wait()
            ws_in.wait()
        neigh_ref[rows, :] = nt_dot(hidden, wn_ref[...]).astype(bf16)
        if b < 2:
            own_ref[rows, :] = nt_dot(hidden, ws_ref[...])
        if b == 2 - 1:
            own_out.start()
    neigh_out.start()
    pick = one_hot(spread, neigh_ref.shape[0])
    halo_ref[...] = jnp.dot(pick, neigh_ref[...], preferred_element_type=f32).astype(bf16)
    own_out.wait()
    neigh_out.wait()


def second_layer(pre, stat, gain, shift, send, ws, wn, total_rows):
    rows, hidden = pre.shape
    classes = ws.shape[0]
    halo = send.shape[1]
    dma = pltpu.SemaphoreType.DMA
    return pl.pallas_call(
        functools.partial(second_layer_kernel, total_rows=total_rows),
        in_specs=[HBM, VM, VM, VM, VM, HBM, HBM],
        out_specs=[HBM, HBM, VM],
        out_shape=[
            pltpu.HBM((BLOCK, classes), f32),
            pltpu.HBM((rows, classes), bf16),
            jax.ShapeDtypeStruct((halo, classes), bf16),
        ],
        scratch_shapes=[
            pltpu.VMEM(pre.shape, f32),
            pltpu.VMEM(ws.shape, bf16),
            pltpu.VMEM(wn.shape, bf16),
            pltpu.VMEM((BLOCK, classes), f32),
            pltpu.VMEM((rows, classes), bf16),
            dma((rows // (BLOCK // 2),)),
            dma,
            dma,
            dma,
            dma,
        ],
        compiler_params=params(32),
        name="second_layer",
    )(in_hbm(pre), stat, gain, shift, send, in_hbm(ws), in_hbm(wn))


def targets_kernel(adj_ref, own_hbm, neigh_hbm, part_ref, far_ref, count_ref, own_ref, neigh_ref, own_sem, neigh_sem):
    rows = neigh_ref.shape[0]
    own_in = pltpu.make_async_copy(own_hbm, own_ref, own_sem)
    neigh_in = pltpu.make_async_copy(neigh_hbm, neigh_ref, neigh_sem)
    own_in.start()
    neigh_in.start()
    count_neighbours(adj_ref, count_ref)
    own_in.wait()
    neigh_in.wait()
    total = jnp.dot(count_ref[:, :rows], neigh_ref[...], preferred_element_type=f32)
    part_ref[...] = own_ref[...] + total * (1.0 / adj_ref.shape[1])
    far_ref[...] = count_ref[:, rows:]


def targets_layer(adj, own, neigh, halo):
    count, rows = adj.shape[0], neigh.shape[0]
    return pl.pallas_call(
        targets_kernel,
        in_specs=[VM, HBM, HBM],
        out_specs=[VM, VM],
        out_shape=[jax.ShapeDtypeStruct(own.shape, f32), jax.ShapeDtypeStruct((count, halo), bf16)],
        scratch_shapes=[
            pltpu.VMEM((count, rows + halo), bf16),
            pltpu.VMEM(own.shape, f32),
            pltpu.VMEM(neigh.shape, bf16),
            pltpu.SemaphoreType.DMA,
            pltpu.SemaphoreType.DMA,
        ],
        compiler_params=params(16),
        cost_estimate=pl.CostEstimate(
            flops=3 * adj.shape[1] * count * (rows + halo), bytes_accessed=2 * count * rows, transcendentals=0
        ),
        name="targets_layer",
    )(adj, in_hbm(own), in_hbm(neigh))


def output_kernel(part_ref, far_ref, recv_ref, out_ref, *, fanout):
    total = jnp.dot(far_ref[...], recv_ref[...], preferred_element_type=f32)
    out_ref[...] = jnp.transpose(part_ref[...] + total * (1.0 / fanout))


def output(part, far, recv, fanout):
    return pl.pallas_call(
        functools.partial(output_kernel, fanout=fanout),
        in_specs=[VM] * 3,
        out_specs=VM,
        out_shape=jax.ShapeDtypeStruct(part.shape[::-1], f32),
        compiler_params=params(16),
        name="output_layer",
    )(part, far, recv).T


def sum_over(array, axes):
    copies = jnp.broadcast_to(array[None], (lax.axis_size(axes),) + array.shape)
    return jnp.sum(lax.all_to_all(copies, axes, split_axis=0, concat_axis=0, tiled=True), axis=0)


def local(
    hot_rows,
    cold_rows,
    hot_mask,
    hot_id,
    cold_owner,
    cold_pos,
    cold_send,
    adjacency_one,
    adjacency_two,
    halo_send,
    self_first,
    neigh_first,
    bn_gain,
    bn_shift,
    self_second,
    neigh_second,
):
    devices = lax.axis_size(HST_DEV)
    nodes = hot_mask.shape[0]
    fan_one, fan_two = adjacency_one.shape[1], adjacency_two.shape[1]

    outgoing = select_rows(cold_send, cold_rows)
    slots = outgoing.shape[0] // devices
    arrived = lax.all_to_all(outgoing, HST_DEV, split_axis=0, concat_axis=0, tiled=True)

    hot_feat = hot_rows.at[hot_id].get(mode="promise_in_bounds")
    adj_one = counts(adjacency_one, nodes)
    slot = jnp.where(hot_mask == 1, -1, cold_owner * slots + cold_pos)[None, :]

    pre, stat = first_layer(slot, arrived, hot_feat, adj_one, self_first, neigh_first, fan_one)
    stat = sum_over(sum_over(stat, HST), DEV)
    own, neigh, halo = second_layer(
        pre,
        stat,
        bn_gain[None, :],
        bn_shift[None, :],
        halo_send,
        self_second.T,
        neigh_second.T,
        nodes * devices,
    )
    recv = lax.all_to_all(halo, DEV, split_axis=0, concat_axis=0, tiled=True)
    part, far = targets_layer(adjacency_two, own, neigh, halo_send.shape[1])
    return output(part, far, recv, fan_two)


def solution(mesh):
    torus = Mesh(mesh.devices.reshape(4, 2, 4, 4), ("hst_0", "hst_1", "dev_0", "dev_1"))
    split = P(HST_DEV)
    rows = P(HST_DEV, None)
    return jax.shard_map(
        local,
        mesh=torus,
        in_specs=(P(), rows, split, split, split, split, rows, rows, rows, rows, P(), P(), P(), P(), P(), P()),
        out_specs=rows,
        check_vma=False,
    )
```

```python
import functools

import jax
import jax.numpy as jnp
from jax import lax
from jax.experimental import pallas as pl
from jax.experimental.pallas import tpu as pltpu
from jax.sharding import Mesh
from jax.sharding import PartitionSpec as P

HST = ("hst_0", "hst_1")
DEV = ("dev_0", "dev_1")
HST_DEV = ("hst_0", "hst_1", "dev_0", "dev_1")

LANES = 128
BLOCK = 512
epsilon = 1e-05

f32 = jnp.float32
bf16 = jnp.bfloat16


def row_to_lanes(row):
    return jnp.transpose(jnp.broadcast_to(row, (LANES, row.shape[1]))).astype(jnp.int16)


def one_hot(spread, width):
    lane = lax.broadcasted_iota(jnp.int32, spread.shape, 1).astype(jnp.int16)
    one, zero = jnp.array(1, bf16), jnp.array(0, bf16)
    tiles = [
        jnp.where(spread == lane + jnp.int16(LANES * j), one, zero) for j in range(width // LANES)
    ]
    return jnp.concatenate(tiles, axis=1)


VM = pl.BlockSpec(memory_space=pltpu.VMEM)
HBM = pl.BlockSpec(memory_space=pl.ANY)


def resident(array):
    return pltpu.with_memory_space_constraint(array, pltpu.VMEM)


def in_hbm(array):
    return pltpu.with_memory_space_constraint(array, pltpu.HBM)


def params(mib):
    return pltpu.CompilerParams(vmem_limit_bytes=mib * 2**20)


def whole(shape):
    return pl.BlockSpec(shape, lambda i: (0,) * len(shape))


def select_rows_kernel(idx_hbm, table_hbm, out_hbm, idx_ref, table_ref, out_ref, idx_sem, table_sem, out_sem):
    blocks = out_ref.shape[0] // BLOCK
    at = [pl.ds(b * BLOCK, BLOCK) for b in range(blocks)]
    idx_in = pltpu.make_async_copy(idx_hbm, idx_ref, idx_sem)
    table_in = pltpu.make_async_copy(table_hbm, table_ref, table_sem)
    copies = [pltpu.make_async_copy(out_ref.at[at[b]], out_hbm.at[at[b]], out_sem.at[b]) for b in range(blocks)]
    idx_in.start()
    table_in.start()
    idx_in.wait()
    spread = [row_to_lanes(idx_ref[:, at[b]]) for b in range(blocks)]
    table_in.wait()
    for b in range(blocks):
        pick = one_hot(spread[b], table_ref.shape[0])
        out_ref[at[b], :] = jnp.dot(pick, table_ref[...], preferred_element_type=f32).astype(bf16)
        copies[b].start()
    for copy in copies:
        copy.wait()


def select_rows(idx, table):
    rows, width = idx.shape[1], table.shape[1]
    return pl.pallas_call(
        select_rows_kernel,
        in_specs=[HBM, HBM],
        out_specs=HBM,
        out_shape=pltpu.HBM((rows, width), bf16),
        scratch_shapes=[
            pltpu.VMEM(idx.shape, jnp.int32),
            pltpu.VMEM(table.shape, bf16),
            pltpu.VMEM((rows, width), bf16),
            pltpu.SemaphoreType.DMA,
            pltpu.SemaphoreType.DMA,
            pltpu.SemaphoreType.DMA((rows // BLOCK,)),
        ],
        compiler_params=params(24),
        name="select_rows",
    )(in_hbm(idx), in_hbm(table))


def count_neighbours(adj_ref, out_ref):
    step = 16
    group = 8
    fanout = adj_ref.shape[1]
    width = out_ref.shape[1]
    lane = lax.broadcasted_iota(jnp.int32, (step, LANES), 1).astype(jnp.int16)
    one, zero = jnp.array(1, bf16), jnp.array(0, bf16)

    def body(r, carry):
        for g in range(group):
            start = pl.multiple_of((r * group + g) * step, step)
            rows = adj_ref[pl.ds(start, step), :]
            spread = [
                jnp.broadcast_to(rows[:, k : k + 1], (step, LANES)).astype(jnp.int16) for k in range(fanout)
            ]
            for j in range(width // LANES):
                here = lane + jnp.int16(LANES * j)
                acc = jnp.where(spread[0] == here, one, zero)
                for k in range(1, fanout):
                    acc = acc + jnp.where(spread[k] == here, one, zero)
                out_ref[pl.ds(start, step), LANES * j : LANES * (j + 1)] = acc
        return carry

    lax.fori_loop(0, adj_ref.shape[0] // (step * group), body, 0)


def counts(adjacency, width):
    rows, fanout = adjacency.shape
    block = BLOCK // 2
    return pl.pallas_call(
        count_neighbours,
        grid=(rows // block,),
        in_specs=[pl.BlockSpec((block, fanout), lambda i: (i, 0))],
        out_specs=pl.BlockSpec((block, width), lambda i: (i, 0)),
        out_shape=pltpu.HBM((rows, width), bf16),
        compiler_params=params(24),
        cost_estimate=pl.CostEstimate(
            flops=3 * fanout * rows * width, bytes_accessed=2 * rows * width, transcendentals=0
        ),
        name="neighbour_counts",
    )(in_hbm(adjacency))


def first_layer_kernel(
    slot_ref, arrived_ref, hot_hbm, adj_hbm, ws_hbm, wn_hbm, pre_hbm, stat_ref,
    hot_ref, adj_ref, w_ref, pre_ref, hot_sem, adj_sem, ws_sem, wn_sem, pre_sem, both_ref, *, fanout
):
    rows, width = hot_ref.shape
    blocks = rows // BLOCK
    at = [pl.ds(b * BLOCK, BLOCK) for b in range(blocks)]
    out = at[:-1] + [pl.ds(rows - BLOCK, BLOCK // 2), pl.ds(rows - BLOCK // 2, BLOCK // 2)]
    hot_in = pltpu.make_async_copy(hot_hbm, hot_ref, hot_sem)
    adj_in = pltpu.make_async_copy(adj_hbm, adj_ref, adj_sem)
    ws_in = pltpu.make_async_copy(ws_hbm, w_ref.at[pl.ds(0, width)], ws_sem)
    wn_in = pltpu.make_async_copy(wn_hbm, w_ref.at[pl.ds(width, width)], wn_sem)
    pre_out = [pltpu.make_async_copy(pre_ref.at[out[b]], pre_hbm.at[out[b]], pre_sem.at[b]) for b in range(len(out))]
    for copy in (hot_in, adj_in, ws_in, wn_in):
        copy.start()
    for b in range(blocks):
        spread = row_to_lanes(slot_ref[:, at[b]])
        cold = jnp.dot(one_hot(spread, arrived_ref.shape[0]), arrived_ref[...], preferred_element_type=f32).astype(bf16)
        if b == 0:
            hot_in.wait()
        for j in range(width // LANES):
            lanes = slice(LANES * j, LANES * (j + 1))
            both_ref[at[b], lanes] = jnp.where(spread < jnp.int16(0), hot_ref[at[b], lanes], cold[:, lanes])
    adj_in.wait()
    ws_in.wait()
    wn_in.wait()
    for b in range(blocks):
        total = jnp.dot(adj_ref[at[b], :], both_ref[:, :width], preferred_element_type=f32)
        both_ref[at[b], width:] = (total * (1.0 / fanout)).astype(bf16)
    sums = squares = 0
    for b in range(len(out)):
        pre = jnp.dot(both_ref[out[b], :], w_ref[...], preferred_element_type=f32)
        pre_ref[out[b], :] = pre
        pre_out[b].start()
        grouped = pre.reshape(pre.shape[0] // 8, 8, pre.shape[1])
        sums = sums + jnp.sum(grouped, axis=0)
        squares = squares + jnp.sum(grouped * grouped, axis=0)
    stat_ref[0:1, :] = jnp.sum(sums, axis=0, keepdims=True)
    stat_ref[1:2, :] = jnp.sum(squares, axis=0, keepdims=True)
    for copy in pre_out:
        copy.wait()


def first_layer(slot, arrived, hot, adj, ws, wn, fanout):
    rows, width = hot.shape
    hidden = ws.shape[1]
    blocks = rows // BLOCK
    return pl.pallas_call(
        functools.partial(first_layer_kernel, fanout=fanout),
        in_specs=[VM, VM, HBM, HBM, HBM, HBM],
        out_specs=[HBM, VM],
        out_shape=[
            pltpu.HBM((rows, hidden), f32),
            jax.ShapeDtypeStruct((2, hidden), f32),
        ],
        scratch_shapes=[
            pltpu.VMEM(hot.shape, bf16),
            pltpu.VMEM((rows, rows), bf16),
            pltpu.VMEM((2 * width, hidden), bf16),
            pltpu.VMEM((rows, hidden), f32),
            pltpu.SemaphoreType.DMA,
            pltpu.SemaphoreType.DMA,
            pltpu.SemaphoreType.DMA,
            pltpu.SemaphoreType.DMA,
            pltpu.SemaphoreType.DMA((blocks + 1,)),
            pltpu.VMEM((rows, 2 * width), bf16),
        ],
        compiler_params=params(48),
        name="first_layer",
    )(slot, resident(arrived), in_hbm(hot), in_hbm(adj), in_hbm(ws), in_hbm(wn))


def nt_dot(a, b):
    return lax.dot_general(a, b, (((1,), (1,)), ((), ())), preferred_element_type=f32)


def second_layer_kernel(
    pre_hbm, stat_ref, gain_ref, shift_ref, send_ref, ws_hbm, wn_hbm, own_hbm, neigh_hbm, halo_ref,
    pre_ref, ws_ref, wn_ref, own_ref, neigh_ref, pre_sem, ws_sem, wn_sem, own_sem, neigh_sem, *, total_rows
):
    step = BLOCK // 2
    at = [pl.ds(start, step) for start in range(0, pre_ref.shape[0], step)]
    pre_in = [pltpu.make_async_copy(pre_hbm.at[rows], pre_ref.at[rows], pre_sem.at[b]) for b, rows in enumerate(at)]
    ws_in = pltpu.make_async_copy(ws_hbm, ws_ref, ws_sem)
    wn_in = pltpu.make_async_copy(wn_hbm, wn_ref, wn_sem)
    own_out = pltpu.make_async_copy(own_ref, own_hbm, own_sem)
    neigh_out = pltpu.make_async_copy(neigh_ref, neigh_hbm, neigh_sem)
    for copy in [wn_in] + pre_in[:3] + [ws_in]:
        copy.start()
    spread = row_to_lanes(send_ref[...])
    mean = stat_ref[0:1, :] * (1.0 / total_rows)
    variance = stat_ref[1:2, :] * (1.0 / total_rows) - mean * mean
    scale = lax.rsqrt(variance + epsilon) * gain_ref[...]
    shift = shift_ref[...]
    for b, rows in enumerate(at):
        pre_in[b].wait()
        if b + 3 < len(at):
            pre_in[b + 3].start()
        hidden = jnp.maximum((pre_ref[rows, :] - mean) * scale + shift, 0.0).astype(bf16)
        if b == 0:
            wn_in.wait()
            ws_in.wait()
        neigh_ref[rows, :] = nt_dot(hidden, wn_ref[...]).astype(bf16)
        if b < 2:
            own_ref[rows, :] = nt_dot(hidden, ws_ref[...])
        if b == 2 - 1:
            own_out.start()
    neigh_out.start()
    pick = one_hot(spread, neigh_ref.shape[0])
    halo_ref[...] = jnp.dot(pick, neigh_ref[...], preferred_element_type=f32).astype(bf16)
    own_out.wait()
    neigh_out.wait()


def second_layer(pre, stat, gain, shift, send, ws, wn, total_rows):
    rows, hidden = pre.shape
    classes = ws.shape[0]
    halo = send.shape[1]
    dma = pltpu.SemaphoreType.DMA
    return pl.pallas_call(
        functools.partial(second_layer_kernel, total_rows=total_rows),
        in_specs=[HBM, VM, VM, VM, VM, HBM, HBM],
        out_specs=[HBM, HBM, VM],
        out_shape=[
            pltpu.HBM((BLOCK, classes), f32),
            pltpu.HBM((rows, classes), bf16),
            jax.ShapeDtypeStruct((halo, classes), bf16),
        ],
        scratch_shapes=[
            pltpu.VMEM(pre.shape, f32),
            pltpu.VMEM(ws.shape, bf16),
            pltpu.VMEM(wn.shape, bf16),
            pltpu.VMEM((BLOCK, classes), f32),
            pltpu.VMEM((rows, classes), bf16),
            dma((rows // (BLOCK // 2),)),
            dma,
            dma,
            dma,
            dma,
        ],
        compiler_params=params(32),
        name="second_layer",
    )(in_hbm(pre), stat, gain, shift, send, in_hbm(ws), in_hbm(wn))


def targets_kernel(adj_ref, own_hbm, neigh_hbm, part_ref, far_ref, count_ref, own_ref, neigh_ref, own_sem, neigh_sem):
    rows = neigh_ref.shape[0]
    own_in = pltpu.make_async_copy(own_hbm, own_ref, own_sem)
    neigh_in = pltpu.make_async_copy(neigh_hbm, neigh_ref, neigh_sem)
    own_in.start()
    neigh_in.start()
    count_neighbours(adj_ref, count_ref)
    own_in.wait()
    neigh_in.wait()
    total = jnp.dot(count_ref[:, :rows], neigh_ref[...], preferred_element_type=f32)
    part_ref[...] = own_ref[...] + total * (1.0 / adj_ref.shape[1])
    far_ref[...] = count_ref[:, rows:]


def targets_layer(adj, own, neigh, halo):
    count, rows = adj.shape[0], neigh.shape[0]
    return pl.pallas_call(
        targets_kernel,
        in_specs=[VM, HBM, HBM],
        out_specs=[VM, VM],
        out_shape=[jax.ShapeDtypeStruct(own.shape, f32), jax.ShapeDtypeStruct((count, halo), bf16)],
        scratch_shapes=[
            pltpu.VMEM((count, rows + halo), bf16),
            pltpu.VMEM(own.shape, f32),
            pltpu.VMEM(neigh.shape, bf16),
            pltpu.SemaphoreType.DMA,
            pltpu.SemaphoreType.DMA,
        ],
        compiler_params=params(16),
        cost_estimate=pl.CostEstimate(
            flops=3 * adj.shape[1] * count * (rows + halo), bytes_accessed=2 * count * rows, transcendentals=0
        ),
        name="targets_layer",
    )(adj, in_hbm(own), in_hbm(neigh))


def output_kernel(part_ref, far_ref, recv_ref, out_ref, *, fanout):
    total = jnp.dot(far_ref[...], recv_ref[...], preferred_element_type=f32)
    out_ref[...] = jnp.transpose(part_ref[...] + total * (1.0 / fanout))


def output(part, far, recv, fanout):
    return pl.pallas_call(
        functools.partial(output_kernel, fanout=fanout),
        in_specs=[VM] * 3,
        out_specs=VM,
        out_shape=jax.ShapeDtypeStruct(part.shape[::-1], f32),
        compiler_params=params(16),
        name="output_layer",
    )(part, far, recv).T


def sum_over(array, axes):
    copies = jnp.broadcast_to(array[None], (lax.axis_size(axes),) + array.shape)
    return jnp.sum(lax.all_to_all(copies, axes, split_axis=0, concat_axis=0, tiled=True), axis=0)


def local(
    hot_rows,
    cold_rows,
    hot_mask,
    hot_id,
    cold_owner,
    cold_pos,
    cold_send,
    adjacency_one,
    adjacency_two,
    halo_send,
    self_first,
    neigh_first,
    bn_gain,
    bn_shift,
    self_second,
    neigh_second,
):
    devices = lax.axis_size(HST_DEV)
    nodes = hot_mask.shape[0]
    fan_one, fan_two = adjacency_one.shape[1], adjacency_two.shape[1]

    outgoing = select_rows(cold_send, cold_rows)
    slots = outgoing.shape[0] // devices
    arrived = lax.all_to_all(outgoing, HST_DEV, split_axis=0, concat_axis=0, tiled=True)

    hot_feat = hot_rows.at[hot_id].get(mode="promise_in_bounds")
    adj_one = counts(adjacency_one, nodes)
    slot = jnp.where(hot_mask == 1, -1, cold_owner * slots + cold_pos)[None, :]

    pre, stat = first_layer(slot, arrived, hot_feat, adj_one, self_first, neigh_first, fan_one)
    stat = sum_over(sum_over(stat, HST), DEV)
    own, neigh, halo = second_layer(
        pre,
        stat,
        bn_gain[None, :],
        bn_shift[None, :],
        halo_send,
        self_second.T,
        neigh_second.T,
        nodes * devices,
    )
    recv = lax.all_to_all(halo, DEV, split_axis=0, concat_axis=0, tiled=True)
    part, far = targets_layer(adjacency_two, own, neigh, halo_send.shape[1])
    return output(part, far, recv, fan_two)


def solution(mesh):
    torus = Mesh(mesh.devices.reshape(4, 2, 4, 4), ("hst_0", "hst_1", "dev_0", "dev_1"))
    split = P(HST_DEV)
    rows = P(HST_DEV, None)
    return jax.shard_map(
        local,
        mesh=torus,
        in_specs=(P(), rows, split, split, split, split, rows, rows, rows, rows, P(), P(), P(), P(), P(), P()),
        out_specs=rows,
        check_vma=False,
    )
```

```python
import functools

import jax
import jax.numpy as jnp
from jax import lax
from jax.experimental import pallas as pl
from jax.experimental.pallas import tpu as pltpu
from jax.sharding import Mesh
from jax.sharding import PartitionSpec as P

HST = ("hst_0", "hst_1")
DEV = ("dev_0", "dev_1")
HST_DEV = ("hst_0", "hst_1", "dev_0", "dev_1")

LANES = 128
BLOCK = 512
epsilon = 1e-05

f32 = jnp.float32
bf16 = jnp.bfloat16


def row_to_lanes(row):
    return jnp.transpose(jnp.broadcast_to(row, (LANES, row.shape[1]))).astype(jnp.int16)


def one_hot(spread, width):
    lane = lax.broadcasted_iota(jnp.int32, spread.shape, 1).astype(jnp.int16)
    one, zero = jnp.array(1, bf16), jnp.array(0, bf16)
    tiles = [
        jnp.where(spread == lane + jnp.int16(LANES * j), one, zero) for j in range(width // LANES)
    ]
    return jnp.concatenate(tiles, axis=1)


VM = pl.BlockSpec(memory_space=pltpu.VMEM)
HBM = pl.BlockSpec(memory_space=pl.ANY)


def resident(array):
    return pltpu.with_memory_space_constraint(array, pltpu.VMEM)


def in_hbm(array):
    return pltpu.with_memory_space_constraint(array, pltpu.HBM)


def params(mib):
    return pltpu.CompilerParams(vmem_limit_bytes=mib * 2**20)


def whole(shape):
    return pl.BlockSpec(shape, lambda i: (0,) * len(shape))


def select_rows_kernel(idx_hbm, table_hbm, out_hbm, idx_ref, table_ref, out_ref, idx_sem, table_sem, out_sem):
    rows = out_ref.shape[0]
    at = [pl.ds(b, BLOCK) for b in range(0, rows - BLOCK, BLOCK)]
    at += [pl.ds(rows - BLOCK, BLOCK // 2), pl.ds(rows - BLOCK // 2, BLOCK // 2)]
    blocks = len(at)
    idx_in = pltpu.make_async_copy(idx_hbm, idx_ref, idx_sem)
    table_in = pltpu.make_async_copy(table_hbm, table_ref, table_sem)
    copies = [pltpu.make_async_copy(out_ref.at[at[b]], out_hbm.at[at[b]], out_sem.at[b]) for b in range(blocks)]
    idx_in.start()
    table_in.start()
    idx_in.wait()
    spread = [row_to_lanes(idx_ref[:, at[b]]) for b in range(blocks)]
    table_in.wait()
    for b in range(blocks):
        pick = one_hot(spread[b], table_ref.shape[0])
        out_ref[at[b], :] = jnp.dot(pick, table_ref[...], preferred_element_type=f32).astype(bf16)
        copies[b].start()
    for copy in copies:
        copy.wait()


def select_rows(idx, table):
    rows, width = idx.shape[1], table.shape[1]
    return pl.pallas_call(
        select_rows_kernel,
        in_specs=[HBM, HBM],
        out_specs=HBM,
        out_shape=pltpu.HBM((rows, width), bf16),
        scratch_shapes=[
            pltpu.VMEM(idx.shape, jnp.int32),
            pltpu.VMEM(table.shape, bf16),
            pltpu.VMEM((rows, width), bf16),
            pltpu.SemaphoreType.DMA,
            pltpu.SemaphoreType.DMA,
            pltpu.SemaphoreType.DMA((rows // BLOCK + 1,)),
        ],
        compiler_params=params(24),
        name="select_rows",
    )(in_hbm(idx), in_hbm(table))


def count_neighbours(adj_ref, out_ref):
    step = 16
    group = 8
    fanout = adj_ref.shape[1]
    width = out_ref.shape[1]
    lane = lax.broadcasted_iota(jnp.int32, (step, LANES), 1).astype(jnp.int16)
    one, zero = jnp.array(1, bf16), jnp.array(0, bf16)

    def body(r, carry):
        for g in range(group):
            start = pl.multiple_of((r * group + g) * step, step)
            rows = adj_ref[pl.ds(start, step), :]
            spread = [
                jnp.broadcast_to(rows[:, k : k + 1], (step, LANES)).astype(jnp.int16) for k in range(fanout)
            ]
            for j in range(width // LANES):
                here = lane + jnp.int16(LANES * j)
                acc = jnp.where(spread[0] == here, one, zero)
                for k in range(1, fanout):
                    acc = acc + jnp.where(spread[k] == here, one, zero)
                out_ref[pl.ds(start, step), LANES * j : LANES * (j + 1)] = acc
        return carry

    lax.fori_loop(0, adj_ref.shape[0] // (step * group), body, 0)


def counts(adjacency, width):
    rows, fanout = adjacency.shape
    block = BLOCK // 2
    return pl.pallas_call(
        count_neighbours,
        grid=(rows // block,),
        in_specs=[pl.BlockSpec((block, fanout), lambda i: (i, 0))],
        out_specs=pl.BlockSpec((block, width), lambda i: (i, 0)),
        out_shape=pltpu.HBM((rows, width), bf16),
        compiler_params=params(24),
        cost_estimate=pl.CostEstimate(
            flops=3 * fanout * rows * width, bytes_accessed=2 * rows * width, transcendentals=0
        ),
        name="neighbour_counts",
    )(in_hbm(adjacency))


def first_layer_kernel(
    slot_ref, arrived_ref, hot_hbm, adj_hbm, ws_hbm, wn_hbm, pre_hbm, stat_ref,
    hot_ref, adj_ref, w_ref, pre_ref, hot_sem, adj_sem, ws_sem, wn_sem, pre_sem, both_ref, *, fanout
):
    rows, width = hot_ref.shape
    blocks = rows // BLOCK
    at = [pl.ds(b * BLOCK, BLOCK) for b in range(blocks)]
    out = at[:-1] + [pl.ds(rows - BLOCK + c * LANES, LANES) for c in range(BLOCK // LANES)]
    hot_in = pltpu.make_async_copy(hot_hbm, hot_ref, hot_sem)
    adj_in = pltpu.make_async_copy(adj_hbm, adj_ref, adj_sem)
    ws_in = pltpu.make_async_copy(ws_hbm, w_ref.at[pl.ds(0, width)], ws_sem)
    wn_in = pltpu.make_async_copy(wn_hbm, w_ref.at[pl.ds(width, width)], wn_sem)
    pre_out = [pltpu.make_async_copy(pre_ref.at[out[b]], pre_hbm.at[out[b]], pre_sem.at[b]) for b in range(len(out))]
    for copy in (hot_in, adj_in, ws_in, wn_in):
        copy.start()
    for b in range(blocks):
        spread = row_to_lanes(slot_ref[:, at[b]])
        cold = jnp.dot(one_hot(spread, arrived_ref.shape[0]), arrived_ref[...], preferred_element_type=f32).astype(bf16)
        if b == 0:
            hot_in.wait()
        for j in range(width // LANES):
            lanes = slice(LANES * j, LANES * (j + 1))
            both_ref[at[b], lanes] = jnp.where(spread < jnp.int16(0), hot_ref[at[b], lanes], cold[:, lanes])
    adj_in.wait()
    ws_in.wait()
    wn_in.wait()
    for b in range(blocks):
        total = jnp.dot(adj_ref[at[b], :], both_ref[:, :width], preferred_element_type=f32)
        both_ref[at[b], width:] = (total * (1.0 / fanout)).astype(bf16)
    sums = squares = 0
    for b in range(len(out)):
        pre = jnp.dot(both_ref[out[b], :], w_ref[...], preferred_element_type=f32)
        pre_ref[out[b], :] = pre
        pre_out[b].start()
        grouped = pre.reshape(pre.shape[0] // 8, 8, pre.shape[1])
        sums = sums + jnp.sum(grouped, axis=0)
        squares = squares + jnp.sum(grouped * grouped, axis=0)
    stat_ref[0:1, :] = jnp.sum(sums, axis=0, keepdims=True)
    stat_ref[1:2, :] = jnp.sum(squares, axis=0, keepdims=True)
    for copy in pre_out:
        copy.wait()


def first_layer(slot, arrived, hot, adj, ws, wn, fanout):
    rows, width = hot.shape
    hidden = ws.shape[1]
    blocks = rows // BLOCK
    return pl.pallas_call(
        functools.partial(first_layer_kernel, fanout=fanout),
        in_specs=[VM, VM, HBM, HBM, HBM, HBM],
        out_specs=[HBM, VM],
        out_shape=[
            pltpu.HBM((rows, hidden), f32),
            jax.ShapeDtypeStruct((2, hidden), f32),
        ],
        scratch_shapes=[
            pltpu.VMEM(hot.shape, bf16),
            pltpu.VMEM((rows, rows), bf16),
            pltpu.VMEM((2 * width, hidden), bf16),
            pltpu.VMEM((rows, hidden), f32),
            pltpu.SemaphoreType.DMA,
            pltpu.SemaphoreType.DMA,
            pltpu.SemaphoreType.DMA,
            pltpu.SemaphoreType.DMA,
            pltpu.SemaphoreType.DMA((blocks - 1 + BLOCK // LANES,)),
            pltpu.VMEM((rows, 2 * width), bf16),
        ],
        compiler_params=params(48),
        name="first_layer",
    )(slot, resident(arrived), in_hbm(hot), in_hbm(adj), in_hbm(ws), in_hbm(wn))


def nt_dot(a, b):
    return lax.dot_general(a, b, (((1,), (1,)), ((), ())), preferred_element_type=f32)


def second_layer_kernel(
    pre_hbm, stat_ref, gain_ref, shift_ref, send_ref, ws_hbm, wn_hbm, own_hbm, neigh_hbm, halo_ref,
    pre_ref, ws_ref, wn_ref, own_ref, neigh_ref, pre_sem, ws_sem, wn_sem, own_sem, neigh_sem, *, total_rows
):
    step = BLOCK // 2
    at = [pl.ds(start, step) for start in range(0, pre_ref.shape[0], step)]
    pre_in = [pltpu.make_async_copy(pre_hbm.at[rows], pre_ref.at[rows], pre_sem.at[b]) for b, rows in enumerate(at)]
    ws_in = pltpu.make_async_copy(ws_hbm, ws_ref, ws_sem)
    wn_in = pltpu.make_async_copy(wn_hbm, wn_ref, wn_sem)
    own_out = pltpu.make_async_copy(own_ref, own_hbm, own_sem)
    neigh_out = pltpu.make_async_copy(neigh_ref, neigh_hbm, neigh_sem)
    for copy in [wn_in] + pre_in[:3] + [ws_in]:
        copy.start()
    spread = row_to_lanes(send_ref[...])
    mean = stat_ref[0:1, :] * (1.0 / total_rows)
    variance = stat_ref[1:2, :] * (1.0 / total_rows) - mean * mean
    scale = lax.rsqrt(variance + epsilon) * gain_ref[...]
    shift = shift_ref[...]
    for b, rows in enumerate(at):
        pre_in[b].wait()
        if b + 3 < len(at):
            pre_in[b + 3].start()
        hidden = jnp.maximum((pre_ref[rows, :] - mean) * scale + shift, 0.0).astype(bf16)
        if b == 0:
            wn_in.wait()
            ws_in.wait()
        neigh_ref[rows, :] = nt_dot(hidden, wn_ref[...]).astype(bf16)
        if b < 2:
            own_ref[rows, :] = nt_dot(hidden, ws_ref[...])
        if b == 2 - 1:
            own_out.start()
    neigh_out.start()
    pick = one_hot(spread, neigh_ref.shape[0])
    halo_ref[...] = jnp.dot(pick, neigh_ref[...], preferred_element_type=f32).astype(bf16)
    own_out.wait()
    neigh_out.wait()


def second_layer(pre, stat, gain, shift, send, ws, wn, total_rows):
    rows, hidden = pre.shape
    classes = ws.shape[0]
    halo = send.shape[1]
    dma = pltpu.SemaphoreType.DMA
    return pl.pallas_call(
        functools.partial(second_layer_kernel, total_rows=total_rows),
        in_specs=[HBM, VM, VM, VM, VM, HBM, HBM],
        out_specs=[HBM, HBM, VM],
        out_shape=[
            pltpu.HBM((BLOCK, classes), f32),
            pltpu.HBM((rows, classes), bf16),
            jax.ShapeDtypeStruct((halo, classes), bf16),
        ],
        scratch_shapes=[
            pltpu.VMEM(pre.shape, f32),
            pltpu.VMEM(ws.shape, bf16),
            pltpu.VMEM(wn.shape, bf16),
            pltpu.VMEM((BLOCK, classes), f32),
            pltpu.VMEM((rows, classes), bf16),
            dma((rows // (BLOCK // 2),)),
            dma,
            dma,
            dma,
            dma,
        ],
        compiler_params=params(32),
        name="second_layer",
    )(in_hbm(pre), stat, gain, shift, send, in_hbm(ws), in_hbm(wn))


def targets_kernel(adj_ref, own_hbm, neigh_hbm, part_ref, far_ref, count_ref, own_ref, neigh_ref, own_sem, neigh_sem):
    rows = neigh_ref.shape[0]
    own_in = pltpu.make_async_copy(own_hbm, own_ref, own_sem)
    neigh_in = pltpu.make_async_copy(neigh_hbm, neigh_ref, neigh_sem)
    own_in.start()
    neigh_in.start()
    count_neighbours(adj_ref, count_ref)
    own_in.wait()
    neigh_in.wait()
    total = jnp.dot(count_ref[:, :rows], neigh_ref[...], preferred_element_type=f32)
    part_ref[...] = own_ref[...] + total * (1.0 / adj_ref.shape[1])
    far_ref[...] = count_ref[:, rows:]


def targets_layer(adj, own, neigh, halo):
    count, rows = adj.shape[0], neigh.shape[0]
    return pl.pallas_call(
        targets_kernel,
        in_specs=[VM, HBM, HBM],
        out_specs=[VM, VM],
        out_shape=[jax.ShapeDtypeStruct(own.shape, f32), jax.ShapeDtypeStruct((count, halo), bf16)],
        scratch_shapes=[
            pltpu.VMEM((count, rows + halo), bf16),
            pltpu.VMEM(own.shape, f32),
            pltpu.VMEM(neigh.shape, bf16),
            pltpu.SemaphoreType.DMA,
            pltpu.SemaphoreType.DMA,
        ],
        compiler_params=params(16),
        cost_estimate=pl.CostEstimate(
            flops=3 * adj.shape[1] * count * (rows + halo), bytes_accessed=2 * count * rows, transcendentals=0
        ),
        name="targets_layer",
    )(adj, in_hbm(own), in_hbm(neigh))


def output_kernel(part_ref, far_ref, recv_ref, out_ref, *, fanout):
    total = jnp.dot(far_ref[...], recv_ref[...], preferred_element_type=f32)
    out_ref[...] = jnp.transpose(part_ref[...] + total * (1.0 / fanout))


def output(part, far, recv, fanout):
    return pl.pallas_call(
        functools.partial(output_kernel, fanout=fanout),
        in_specs=[VM] * 3,
        out_specs=VM,
        out_shape=jax.ShapeDtypeStruct(part.shape[::-1], f32),
        compiler_params=params(16),
        name="output_layer",
    )(part, far, recv).T


def sum_over(array, axes):
    copies = jnp.broadcast_to(array[None], (lax.axis_size(axes),) + array.shape)
    return jnp.sum(lax.all_to_all(copies, axes, split_axis=0, concat_axis=0, tiled=True), axis=0)


def local(
    hot_rows,
    cold_rows,
    hot_mask,
    hot_id,
    cold_owner,
    cold_pos,
    cold_send,
    adjacency_one,
    adjacency_two,
    halo_send,
    self_first,
    neigh_first,
    bn_gain,
    bn_shift,
    self_second,
    neigh_second,
):
    devices = lax.axis_size(HST_DEV)
    nodes = hot_mask.shape[0]
    fan_one, fan_two = adjacency_one.shape[1], adjacency_two.shape[1]

    outgoing = select_rows(cold_send, cold_rows)
    slots = outgoing.shape[0] // devices
    arrived = lax.all_to_all(outgoing, HST_DEV, split_axis=0, concat_axis=0, tiled=True)

    hot_feat = hot_rows.at[hot_id].get(mode="promise_in_bounds")
    adj_one = counts(adjacency_one, nodes)
    slot = jnp.where(hot_mask == 1, -1, cold_owner * slots + cold_pos)[None, :]

    pre, stat = first_layer(slot, arrived, hot_feat, adj_one, self_first, neigh_first, fan_one)
    stat = sum_over(sum_over(stat, HST), DEV)
    own, neigh, halo = second_layer(
        pre,
        stat,
        bn_gain[None, :],
        bn_shift[None, :],
        halo_send,
        self_second.T,
        neigh_second.T,
        nodes * devices,
    )
    recv = lax.all_to_all(halo, DEV, split_axis=0, concat_axis=0, tiled=True)
    part, far = targets_layer(adjacency_two, own, neigh, halo_send.shape[1])
    return output(part, far, recv, fan_two)


def solution(mesh):
    torus = Mesh(mesh.devices.reshape(4, 2, 4, 4), ("hst_0", "hst_1", "dev_0", "dev_1"))
    split = P(HST_DEV)
    rows = P(HST_DEV, None)
    return jax.shard_map(
        local,
        mesh=torus,
        in_specs=(P(), rows, split, split, split, split, rows, rows, rows, rows, P(), P(), P(), P(), P(), P()),
        out_specs=rows,
        check_vma=False,
    )
```
